256 devices in a mesh: node: 64 (over z, y_lo, x), expert: 4 (over y_hi, core).
Axes of the slice: x: 4, y: 4 (y_hi: 2, y_lo: 2; y = y_hi * 2 + y_lo), z: 8, core: 2. Of those that a mesh axis runs over, the one named last changes fastest.
Arguments:
- param_gu: float32 [262144, 1024], P('node', 'expert'), may hold values from -13 to 13
- param_down: float32 [8192, 16384], P('node', 'expert'), may hold values from -13 to 13
- tokens: bfloat16 [32768, 4096], P(('node', 'expert')), may hold values from -6 to 6
- cotangent: bfloat16 [32768, 4096], P(('node', 'expert')), may hold values from -6 to 6
- routes: int32 [32768, 2], P(('node', 'expert')), may hold values from 0 to 3, all different within a row; in each aligned block of 128 rows (0 to 127, 128 to 255, ...) at most 96 rows name the same one
- plan: int32 [4], replicated, may hold values from 0 to 5
Outputs:
- gossiped_gu: bfloat16 [262144, 1024], P('node', 'expert')
- gossiped_down: bfloat16 [8192, 16384], P('node', 'expert')
- averaged_gu: float32 [4096, 1024], P('node', 'expert')
- averaged_down: float32 [128, 16384], P('node', 'expert')
The draws below stay inside these ranges and needn't reach their ends.
Inputs may be any that keep to these rules, and one draw needn't show every extreme that they name: `routes`: each row names 2 different experts; the rows of one device name one expert 96 times at most.
All inputs are finite; a program needn't handle non-finite values.
Results may differ from the reference program's by a relative error of at most 0.0078.
Values may be sent and summed in bfloat16 or wider, within the bound.
A program may use at most 128 MiB of HBM per device.

```python
import math
import jax
import jax.numpy as jnp
import numpy as np
from jax import lax

D = 4096
H = 128
TOK_DEV = 128
TOP = 2
ROUNDS = 4
SHIFTS = 6
CAP = 96
EXPERTS = 4
TOKENS = 32768
N_NODE = 64


def replica_field(key, per_node, columns):
    total = N_NODE * per_node
    replica = (jnp.arange(total, dtype=jnp.int32) // per_node).astype(jnp.float32)
    frac = (replica / max(N_NODE - 1, 1))[:, None]
    noise = jnp.clip(jax.random.normal(key, (total, columns), jnp.float32), -4.0, 4.0)
    scale = 1.0 + 2.0 * frac
    offset = frac - 0.5
    return scale * noise + offset


def draw_param_gu(key, part):
    return replica_field(jax.random.fold_in(key, 11), D, EXPERTS * 2 * H)


def draw_param_down(key, part):
    return replica_field(jax.random.fold_in(key, 23), H, EXPERTS * D)


def touch_ends(drawn, key, least, largest):
    spot = [jax.random.randint(jax.random.fold_in(key, axis), (), 0, length) for axis, length in enumerate(drawn.shape)]
    widest = drawn.shape.index(max(drawn.shape))
    next_to = spot[:widest] + [(spot[widest] + 1) % drawn.shape[widest]] + spot[widest + 1:]
    return drawn.at[tuple(spot)].set(least).at[tuple(next_to)].set(largest)


def levels(key, extent, pieces, smallest, top_value):
    gain = 1.0
    for axis_at, shards_of in pieces:
        draws = jax.random.uniform(jax.random.fold_in(jax.random.fold_in(key, 6), axis_at), (shards_of,), jnp.float32, smallest / len(pieces), top_value / len(pieces))
        gain = gain * jnp.repeat(jnp.exp(draws), extent[axis_at] // shards_of).reshape((-1,) + (1,) * (len(extent) - 1 - axis_at))
    return gain


def deal_out(stream_key, own, number, rows, number_of, top, most, skew):
    ranking = jax.random.permutation(stream_key, number_of)
    crowded, common = shares(number_of, rows * top, most, skew, True), shares(number_of, rows * top, most, skew, False)
    places = jnp.arange(number_of)

    def named(lengths, offset_by):
        used = int((lengths > 0).sum())
        fixed = max(1, used // 4)
        moved = fixed + (places - fixed + offset_by * (used - fixed)) % max(1, number_of - fixed)
        return jnp.zeros((number_of,), jnp.int32).at[ranking[jnp.where(places < fixed, places, moved)]].set(jnp.asarray(lengths, jnp.int32))

    lengths = jnp.where(number % 4 == 0, named(crowded, number // 4), named(common, number - number // 4 - 1))
    mixed = jax.random.permutation(jax.random.fold_in(own, 3), number_of)
    source_of, receiver = mixed[0:number_of // 2 * 2:2], mixed[1:number_of // 2 * 2:2]
    room = jnp.minimum(lengths[source_of] - 1, most - lengths[receiver]) // 2
    room = jnp.where((source_of == ranking[0]) | (receiver == ranking[0]) | (lengths[receiver] == 0), 0, jnp.maximum(room, 0))
    moved = jax.random.randint(jax.random.fold_in(own, 4), (number_of // 2,), 0, 1 << 20) % (room + 1)
    lengths = lengths.at[source_of].add(-moved).at[receiver].add(moved)
    items = jnp.searchsorted(jnp.cumsum(lengths), jnp.arange(rows * top), side="right").astype(jnp.int32)
    listing = items.reshape(top, rows).T
    listing = listing[jax.random.permutation(jax.random.fold_in(own, 1), rows)]
    offset_by = jax.random.randint(jax.random.fold_in(own, 2), (rows, 1), 0, top)
    return jnp.take_along_axis(listing, (jnp.arange(top)[None, :] + offset_by) % top, axis=1)


def shares(count, total, bound, lean, full):
    loads = [(1 << 20) // math.isqrt(rank ** lean) + 1 for rank in range(1, count + 1)]
    largest = bound if full else min(bound, max(-(-total // count), total * loads[0] // sum(loads)))
    least = 1 if total - largest >= count - 1 else 0
    counts, rest = [largest] + [least] * (count - 1), total - largest - least * (count - 1)
    while rest > 0:
        free = [i for i in range(1, count) if counts[i] < largest] or [i for i in range(1, count) if counts[i] < bound]
        whole, remaining = sum([loads[i] for i in free]), rest
        for i in free:
            addition = min(bound - counts[i], max(1, remaining * loads[i] // whole), rest)
            counts[i] = counts[i] + addition
            rest = rest - addition
    return np.array(counts)


def normal_values(key, dims, spread, bound, shards=(), held_as=jnp.bfloat16):
    level = levels(key, dims, shards, -0.22, 0.18) if shards else 1.0
    entries = jax.random.normal(key, dims, jnp.float32) * spread * level
    return jnp.minimum(jnp.maximum(entries, -bound), bound).astype(held_as)


def setup_inputs(seed: int = 0) -> dict:
    arg_keys = jax.random.split(jax.random.key(seed), 7)
    param_gu = draw_param_gu(jax.random.fold_in(arg_keys[6], 71), 0)
    param_down = draw_param_down(jax.random.fold_in(arg_keys[6], 71), 0)
    tokens = normal_values(arg_keys[2], (TOKENS, D), 1.0, 6.0, ((0, 256),))
    cotangent = normal_values(arg_keys[3], (TOKENS, D), 1.0, 6.0, ((0, 256),))
    routes_keys = jax.random.split(jax.random.fold_in(arg_keys[4], 1), TOKENS // TOK_DEV)
    routes_turns = jax.random.permutation(jax.random.fold_in(arg_keys[4], 3), TOKENS // TOK_DEV)
    routes = jax.vmap(lambda own, number: deal_out(jax.random.fold_in(arg_keys[4], 2), own, number, TOK_DEV, EXPERTS, TOP, CAP, 2))(routes_keys, routes_turns).reshape((TOKENS, TOP))
    plan = touch_ends(jax.random.randint(arg_keys[5], (ROUNDS,), 0, SHIFTS), jax.random.fold_in(arg_keys[5], 1), 0, SHIFTS - 1).astype(jnp.int32)
    return {"param_gu": param_gu, "param_down": param_down, "tokens": tokens, "cotangent": cotangent, "routes": routes, "plan": plan}


def expert_grads(rows, douts, wgu, wdown):
    hid = wdown.shape[0]
    width = rows.shape[1]
    both = jnp.dot(rows, wgu, preferred_element_type=jnp.float32) * (1.0 / math.sqrt(width))
    gate = both[:, :hid]
    upper = both[:, hid:]
    sigma = jax.nn.sigmoid(gate)
    act = (gate * sigma * upper).astype(jnp.bfloat16)
    dact = jnp.dot(douts, wdown.T, preferred_element_type=jnp.float32) * (1.0 / math.sqrt(hid))
    dgate = dact * upper * sigma * (1.0 + gate * (1.0 - sigma))
    dupper = dact * gate * sigma
    dboth = jnp.concatenate([dgate, dupper], axis=1).astype(jnp.bfloat16)
    grad_down = jnp.dot(act.T, douts, preferred_element_type=jnp.float32) * (1.0 / math.sqrt(hid))
    grad_gu = jnp.dot(rows.T, dboth, preferred_element_type=jnp.float32) * (1.0 / math.sqrt(width))
    return (grad_gu, grad_down)

def reference(param_gu, param_down, tokens, cotangent, routes, plan):
    nodes = N_NODE
    groups = EXPERTS
    hid = H
    width = D
    gu_all = param_gu.reshape(nodes, width, groups, 2 * hid)
    down_all = param_down.reshape(nodes, hid, groups, width)
    tok_all = tokens.reshape(nodes, -1, width)
    cot_all = cotangent.reshape(nodes, -1, width)
    route_all = routes.reshape(nodes, -1, TOP)

    def per_node(items):
        gu_node, down_node, inputs, douts, chosen = items
        new_gu = []
        new_down = []
        for expert in range(groups):
            picked = jnp.any(chosen == expert, axis=1)[:, None]
            rows = jnp.where(picked, inputs, jnp.zeros_like(inputs))
            drows = jnp.where(picked, douts, jnp.zeros_like(douts))
            grad_gu, grad_down = expert_grads(rows, drows, gu_node[:, expert].astype(jnp.bfloat16), down_node[:, expert].astype(jnp.bfloat16))
            new_gu.append(gu_node[:, expert] - 0.5 * grad_gu)
            new_down.append(down_node[:, expert] - 0.5 * grad_down)
        return (jnp.stack(new_gu, axis=1), jnp.stack(new_down, axis=1))
    state_gu, state_down = lax.map(per_node, (gu_all, down_all, tok_all, cot_all, route_all))
    ranks = jnp.arange(nodes, dtype=jnp.int32)
    for step in range(ROUNDS):
        shift_by = jnp.left_shift(jnp.int32(1), plan[step].astype(jnp.int32))
        peer = ((ranks + shift_by) % nodes).astype(jnp.int32)
        recv_gu = lax.optimization_barrier(state_gu[peer].astype(jnp.bfloat16)).astype(jnp.float32)
        recv_down = lax.optimization_barrier(state_down[peer].astype(jnp.bfloat16)).astype(jnp.float32)
        state_gu = (state_gu + recv_gu) * 0.5
        state_down = (state_down + recv_down) * 0.5
    gossiped_gu = state_gu.astype(jnp.bfloat16).reshape(nodes * width, groups * 2 * hid)
    gossiped_down = state_down.astype(jnp.bfloat16).reshape(nodes * hid, groups * width)
    averaged_gu = (lax.optimization_barrier(jnp.sum(state_gu, axis=0)) / nodes).reshape(width, groups * 2 * hid)
    averaged_down = (lax.optimization_barrier(jnp.sum(state_down, axis=0)) / nodes).reshape(hid, groups * width)
    return (gossiped_gu, gossiped_down, averaged_gu, averaged_down)
```

```python
import math

import jax
import jax.numpy as jnp
from jax import lax
from jax.experimental import pallas as pl
from jax.experimental.pallas import tpu as pltpu
from jax.sharding import PartitionSpec as P

MESH = pl.DeviceIdType.MESH
ROUNDS = 4
CHUNKS = 3


def expert_step(x, dy, picked, param_gu, param_down):
    hid, width = param_down.shape
    wgu = param_gu.astype(jnp.bfloat16)
    wdown = param_down.astype(jnp.bfloat16)
    both = jnp.dot(x, wgu, preferred_element_type=jnp.float32) * (1.0 / math.sqrt(width))
    gate = both[:, :hid]
    upper = both[:, hid:]
    sigma = jax.nn.sigmoid(gate)
    zero = jnp.zeros((), jnp.float32)
    act = jnp.where(picked, gate * sigma * upper, zero).astype(jnp.bfloat16)
    dact = lax.dot_general(
        dy, wdown, (((1,), (1,)), ((), ())), preferred_element_type=jnp.float32
    ) * (1.0 / math.sqrt(hid))
    dgate = dact * upper * sigma * (1.0 + gate * (1.0 - sigma))
    dupper = dact * gate * sigma
    dboth = jnp.where(picked, jnp.concatenate([dgate, dupper], axis=1), zero).astype(jnp.bfloat16)
    grad_down = lax.dot_general(
        act, dy, (((0,), (0,)), ((), ())), preferred_element_type=jnp.float32
    ) * (1.0 / math.sqrt(hid))
    grad_gu = lax.dot_general(
        x, dboth, (((0,), (0,)), ((), ())), preferred_element_type=jnp.float32
    ) * (1.0 / math.sqrt(width))
    return param_gu - 0.5 * grad_gu, param_down - 0.5 * grad_down


def gossip_kernel(
    nodes, zs, ys, xs, shifts, src, out, mean, half, done, send1, recv1, send2, recv2, keep, *gots
):
    me = lax.axis_index("node")
    rows = src.shape[1] // CHUNKS
    z, y, x = me // (ys * xs), (me // xs) % ys, me % xs

    def peer_at(t):
        j, k = t % zs, t // zs
        dz = (j % 2) * ((j + 1) // 2) + (1 - j % 2) * (zs - j // 2)
        dy, dx = k // xs, k % xs
        return ((z + dz) % zs) * (ys * xs) + ((y + dy) % ys) * xs + (x + dx) % xs

    barrier = pltpu.get_barrier_semaphore()

    @pl.loop(1, nodes)
    def _(t):
        pl.semaphore_signal(barrier, inc=1, device_id={"node": peer_at(t)}, device_id_type=MESH)

    pl.semaphore_wait(barrier, nodes - 1)

    def part(ref, index, c):
        return ref.at[index, pl.ds(c * rows, rows)]

    def first(t, c):
        peer = peer_at(t)
        return pltpu.make_async_remote_copy(
            src_ref=part(src, peer, c),
            dst_ref=gots[c].at[me],
            send_sem=send1.at[c],
            recv_sem=recv1.at[c],
            device_id={"node": peer},
            device_id_type=MESH,
        )

    def second(t, c):
        peer = peer_at(t)
        return pltpu.make_async_remote_copy(
            src_ref=part(done, peer, c),
            dst_ref=part(out, me, c),
            send_sem=send2.at[c],
            recv_sem=recv2.at[c],
            device_id={"node": peer},
            device_id_type=MESH,
        )

    def all_of(c, send, recv):
        most = gots[c].at[pl.ds(0, nodes - 1)]
        return pltpu.make_async_remote_copy(
            src_ref=most,
            dst_ref=most,
            send_sem=send.at[c],
            recv_sem=recv.at[c],
            device_id={"node": (me + 1) % nodes},
            device_id_type=MESH,
        )

    for c in range(CHUNKS):

        @pl.loop(1, nodes)
        def _(t):
            first(t, c).start()

        gots[c][me] = src[me, pl.ds(c * rows, rows)]

    for c in range(CHUNKS):
        span = pl.ds(c * rows, rows)
        all_of(c, send1, recv1).wait_recv()
        s0, s1, s2, s3 = shifts[0], shifts[1], shifts[2], shifts[3]

        def wide(index):
            return gots[c][lax.rem(index, nodes)].astype(jnp.float32)

        def early(n, total):
            own = wide(n)
            half[n] = (own + wide(n + s0)) + (wide(n + s1) + wide(n + s0 + s1))
            return total + own

        total = lax.fori_loop(0, nodes, early, jnp.zeros(half.shape[1:], jnp.float32))
        mean[span] = total * (1.0 / nodes)

        def late(n, carry):
            value = (half[n] + half[lax.rem(n + s2, nodes)]) + (
                half[lax.rem(n + s3, nodes)] + half[lax.rem(n + s2 + s3, nodes)]
            )
            done[n, span] = (value * (1.0 / 16.0)).astype(done.dtype)
            return carry

        lax.fori_loop(0, nodes, late, 0)

        @pl.loop(1, nodes)
        def _(t):
            second(t, c).start()

        pltpu.make_async_copy(part(done, me, c), part(out, me, c), keep.at[c]).start()

    for c in range(CHUNKS):
        all_of(c, send1, recv1).wait_send()
        all_of(c, send2, recv2).wait_send()
        all_of(c, send2, recv2).wait_recv()
        pltpu.make_async_copy(part(done, me, c), part(out, me, c), keep.at[c]).wait()


def gossip(packed, shifts, nodes):
    _, rows, lanes = packed.shape
    ys, xs = 2, 4
    zs = nodes // (ys * xs)

    def body(*refs):
        gossip_kernel(nodes, zs, ys, xs, *refs)

    return pl.pallas_call(
        body,
        out_shape=(
            jax.ShapeDtypeStruct(packed.shape, jnp.bfloat16),
            jax.ShapeDtypeStruct((rows, lanes), jnp.float32),
        ),
        in_specs=[
            pl.BlockSpec(memory_space=pltpu.SMEM),
            pl.BlockSpec(memory_space=pltpu.VMEM),
        ],
        out_specs=(
            pl.BlockSpec(memory_space=pl.ANY),
            pl.BlockSpec(memory_space=pltpu.VMEM),
        ),
        scratch_shapes=[
            pltpu.VMEM((nodes, rows // CHUNKS, lanes), jnp.float32),
            pltpu.VMEM(packed.shape, jnp.bfloat16),
            pltpu.SemaphoreType.DMA((CHUNKS,)),
            pltpu.SemaphoreType.DMA((CHUNKS,)),
            pltpu.SemaphoreType.DMA((CHUNKS,)),
            pltpu.SemaphoreType.DMA((CHUNKS,)),
            pltpu.SemaphoreType.DMA((CHUNKS,)),
        ]
        + [pltpu.VMEM((nodes, rows // CHUNKS, lanes), jnp.bfloat16)] * CHUNKS,
        compiler_params=pltpu.CompilerParams(
            collective_id=1, has_side_effects=True, vmem_limit_bytes=32 * 1024 * 1024
        ),
        name="gossip",
    )(shifts, packed)


def step(param_gu, param_down, tokens, cotangent, routes, plan):
    nodes = lax.axis_size("node")
    expert = lax.axis_index("expert")
    width, cols = param_gu.shape
    hid = param_down.shape[0]
    x = lax.all_gather(tokens, "expert", axis=0, tiled=True)
    dy = lax.all_gather(cotangent, "expert", axis=0, tiled=True)
    named = lax.all_gather(routes, "expert", axis=0, tiled=True)
    picked = jnp.any(named == expert, axis=1)[:, None]
    new_gu, new_down = expert_step(x, dy, picked, param_gu, param_down)
    own_gu, own_down = width // nodes, hid // nodes
    lanes = cols
    packed = jnp.concatenate(
        [
            new_gu.astype(jnp.bfloat16).reshape(nodes, own_gu, lanes),
            new_down.astype(jnp.bfloat16).reshape(nodes, own_down * width // lanes, lanes),
        ],
        axis=1,
    )
    shifts = jnp.left_shift(jnp.int32(1), plan)
    mixed, mean = gossip(packed, shifts, nodes)
    gossiped_gu = mixed[:, :own_gu].reshape(width, cols)
    gossiped_down = mixed[:, own_gu:].reshape(hid, width)
    averaged_gu = mean[:own_gu]
    averaged_down = mean[own_gu:].reshape(own_down, width)
    return gossiped_gu, gossiped_down, averaged_gu, averaged_down


def solution(mesh):
    both = P(("node", "expert"), None)
    split = P("node", "expert")
    return jax.shard_map(
        step,
        mesh=mesh,
        in_specs=(split, split, both, both, both, P()),
        out_specs=(split, split, split, split),
        check_vma=False,
    )
```

```python
import math

import jax
import jax.numpy as jnp
from jax import lax
from jax.experimental import pallas as pl
from jax.experimental.pallas import tpu as pltpu
from jax.sharding import PartitionSpec as P

MESH = pl.DeviceIdType.MESH
X_PARTS = 2
DY_PARTS = 4
GU_PARTS = 4
LANES = 128
TILE = 512
Y_LO, X_SIZE = 2, 4


def kernel_body(
    nodes,
    shifts,
    code,
    tokens,
    cotangent,
    param_gu,
    param_down,
    out_gu,
    out_down,
    mean_gu,
    mean_down,
    x_all,
    dy_all,
    x_turned,
    gu_wide,
    down_wide,
    gu_short,
    down_short,
    both,
    dact,
    act_turned,
    dboth,
    codes,
    stage,
    half_gu,
    half_down,
    send_gu,
    send_down,
    done_gu,
    done_down,
    local_sem,
    block_sem,
    tok_send,
    tok_recv,
    gu_sem,
    down_sem,
    keep_gu,
    keep_down,
    *landing,
):
    got_gu, got_down = landing[:GU_PARTS], landing[GU_PARTS:]
    me = lax.axis_index("node")
    expert = lax.axis_index("expert")
    experts = lax.axis_size("expert")
    plane = Y_LO * X_SIZE
    zs = nodes // plane
    z, y, x = me // plane, (me // X_SIZE) % Y_LO, me % X_SIZE
    sibling = expert + 1 - 2 * (expert % 2)
    across = (expert + 2) % experts
    rows, width = tokens.shape
    hid = param_down.shape[0]
    gu_rows = send_gu.shape[1]
    gu_part = gu_rows // GU_PARTS
    dy_cols = width // DY_PARTS
    blocks = dy_cols // LANES
    down_part = 2 * blocks

    def z_at(j):
        return (z + (j % 2) * ((j + 1) // 2) + (1 - j % 2) * (zs - j // 2)) % zs

    def peer_at(t):
        k = t // zs
        return z_at(t % zs) * plane + ((y + k // X_SIZE) % Y_LO) * X_SIZE + (x + k % X_SIZE) % X_SIZE

    x_cols = width // X_PARTS
    pieces = (
        [(tokens, x_all, pl.ds(c * x_cols, x_cols)) for c in range(X_PARTS)]
        + [(code, codes, None)]
        + [(cotangent, dy_all, pl.ds(c * dy_cols, dy_cols)) for c in range(DY_PARTS)]
    )

    def source(p):
        src, _, cols = pieces[p]
        return src if cols is None else src.at[:, cols]

    def slot(p, s):
        _, dst, cols = pieces[p]
        if cols is None:
            return dst.at[s]
        return dst.at[pl.ds(s * rows, rows), cols]

    loads = [
        pltpu.make_async_copy(param_gu, gu_wide, local_sem.at[0]),
    ]
    for p in range(len(pieces)):
        loads.append(pltpu.make_async_copy(source(p), slot(p, 0), local_sem.at[1 + p]))
    for load in loads:
        load.start()

    def down_load(b):
        cols = pl.ds(pl.multiple_of(b * LANES, LANES), LANES)
        dst = down_wide.at[pl.ds(pl.multiple_of(b * hid, hid), hid)]
        return pltpu.make_async_copy(param_down.at[:, cols], dst, block_sem.at[b])

    @pl.loop(0, width // LANES)
    def _(b):
        down_load(b).start()

    barrier = pltpu.get_barrier_semaphore()
    for other in (sibling, across):
        pl.semaphore_signal(barrier, inc=1, device_id={"expert": other}, device_id_type=MESH)

    @pl.loop(1, nodes)
    def _(t):
        pl.semaphore_signal(barrier, inc=1, device_id={"node": peer_at(t)}, device_id_type=MESH)

    pl.semaphore_wait(barrier, nodes + 1)

    def token_copy(p, way, src, dst, other):
        return pltpu.make_async_remote_copy(
            src_ref=src,
            dst_ref=dst,
            send_sem=tok_send.at[way, p],
            recv_sem=tok_recv.at[way, p],
            device_id={"expert": other},
            device_id_type=MESH,
        )

    to_sibling = [token_copy(p, 0, source(p), slot(p, 1), sibling) for p in range(len(pieces))]
    to_across = [token_copy(p, 1, source(p), slot(p, 2), across) for p in range(len(pieces))]
    onward = [token_copy(p, 2, slot(p, 2), slot(p, 3), sibling) for p in range(len(pieces))]
    for p in range(len(pieces)):
        to_across[p].start()
        to_sibling[p].start()

    loads[0].wait()

    @pl.loop(0, width // TILE)
    def _(k):
        span = pl.ds(pl.multiple_of(k * TILE, TILE), TILE)
        gu_short[span, :] = gu_wide[span, :].astype(jnp.bfloat16)

    @pl.loop(0, width // LANES)
    def _(b):
        down_load(b).wait()
        cols = pl.ds(pl.multiple_of(b * LANES, LANES), LANES)
        block = down_wide[pl.ds(pl.multiple_of(b * hid, hid), hid), :]
        down_short[:, cols] = block.astype(jnp.bfloat16)

    both[...] = jnp.zeros_like(both)
    dact[...] = jnp.zeros_like(dact)

    def arrive(p):
        to_across[p].wait_recv()
        onward[p].start()
        loads[1 + p].wait()
        to_sibling[p].wait_recv()
        onward[p].wait_recv()

    for p in range(X_PARTS):
        arrive(p)

        @pl.loop(p * (x_cols // TILE), (p + 1) * (x_cols // TILE))
        def _(k):
            span = pl.ds(pl.multiple_of(k * TILE, TILE), TILE)
            both[...] += jnp.dot(
                x_all[:, span], gu_short[span, :], preferred_element_type=jnp.float32
            )

    arrive(X_PARTS)
    bit = jnp.where(
        expert == 0, 1, jnp.where(expert == 1, 2, jnp.where(expert == 2, 4, 8))
    ).astype(jnp.int32)

    def picked_at(s):
        wide = jnp.broadcast_to(codes[s][0:1, :], (rows, rows)).T
        return (wide & bit) != 0

    in_scale = 1.0 / math.sqrt(width)
    hid_scale = 1.0 / math.sqrt(hid)
    first = lax.broadcasted_iota(jnp.int32, (hid, hid), 0)
    second = lax.broadcasted_iota(jnp.int32, (hid, hid), 1)
    wanted = jnp.where(first < hid // 2, 2 * first, 2 * first - (hid - 1))
    order = jnp.where(second == wanted, 1.0, 0.0).astype(jnp.bfloat16)
    for s in range(experts):
        part = pl.ds(s * rows, rows)
        gate = both[part, :hid] * in_scale
        upper = both[part, hid:] * in_scale
        act = jnp.where(picked_at(s), gate * jax.nn.sigmoid(gate) * upper, 0.0)
        act_turned[:, part] = lax.dot_general(
            order,
            act.astype(jnp.bfloat16),
            (((1,), (1,)), ((), ())),
            preferred_element_type=jnp.float32,
        ).astype(jnp.bfloat16)

    @pl.loop(0, width // 256)
    def _(k):
        span = pl.ds(pl.multiple_of(k * 256, 256), 256)
        x_turned[span, :] = x_all[:, span].T

    def exchange(t, src, dst, sems, c):
        return pltpu.make_async_remote_copy(
            src_ref=src,
            dst_ref=dst,
            send_sem=sems.at[0, c],
            recv_sem=sems.at[1, c],
            device_id={"node": t},
            device_id_type=MESH,
        )

    def gu_out(peer, c):
        return exchange(
            peer, send_gu.at[peer, pl.ds(c * gu_part, gu_part)], got_gu[c].at[me], gu_sem, c
        )

    def down_out(peer, c):
        return exchange(peer, send_down.at[c, peer], got_down[c].at[me], down_sem, c)

    for c in range(DY_PARTS):
        arrive(X_PARTS + 1 + c)

        @pl.loop(0, dy_cols // TILE)
        def _(k):
            at = pl.multiple_of(c * dy_cols + k * TILE, TILE)
            span = pl.ds(at, TILE)
            dact[...] += lax.dot_general(
                dy_all[:, span],
                down_short[:, span],
                (((1,), (1,)), ((), ())),
                preferred_element_type=jnp.float32,
            )
            grad = jnp.dot(act_turned[...], dy_all[:, span], preferred_element_type=jnp.float32)
            grad = grad * (0.5 * hid_scale)
            for r in range(2):
                for i in range(TILE // LANES):
                    block = c * blocks + k * (TILE // LANES) + i
                    old = down_wide[pl.ds(block * hid + r, nodes, stride=2), :]
                    new = old - grad[r * nodes : (r + 1) * nodes, i * LANES : (i + 1) * LANES]
                    row = r * blocks + k * (TILE // LANES) + i
                    stage[pl.ds(row, nodes, stride=down_part), :] = new

        @pl.loop(0, nodes)
        def _(n):
            span = pl.ds(pl.multiple_of(n * down_part, down_part), down_part)
            send_down[c, n] = stage[span, :].astype(jnp.bfloat16)

        @pl.loop(1, nodes)
        def _(t):
            down_out(peer_at(t), c).start()

        got_down[c][me] = send_down[c, me]

    for s in range(experts):
        part = pl.ds(s * rows, rows)
        gate = both[part, :hid] * in_scale
        upper = both[part, hid:] * in_scale
        sigma = jax.nn.sigmoid(gate)
        da = dact[part, :] * hid_scale
        picked = picked_at(s)
        dgate = da * upper * sigma * (1.0 + gate * (1.0 - sigma))
        dupper = da * gate * sigma
        dboth[part, :hid] = jnp.where(picked, dgate, 0.0).astype(jnp.bfloat16)
        dboth[part, hid:] = jnp.where(picked, dupper, 0.0).astype(jnp.bfloat16)

    @pl.loop(0, zs)
    def _(j):
        zt = z_at(j)
        at = pl.multiple_of(zt * (plane * gu_rows), plane * gu_rows)
        span = pl.ds(at, plane * gu_rows)
        grad = jnp.dot(x_turned[span, :], dboth[...], preferred_element_type=jnp.float32)
        new = gu_wide[span, :] - grad * (0.5 * in_scale)
        send_gu[pl.ds(zt * plane, plane)] = new.astype(jnp.bfloat16).reshape(
            plane, gu_rows, new.shape[1]
        )

        @pl.loop(0, plane)
        def _(k):
            peer = zt * plane + (me + k) % plane

            @pl.when(peer != me)
            def _():
                gu_out(peer, 0).start()

    for c in range(1, GU_PARTS):

        @pl.loop(1, nodes)
        def _(t):
            gu_out(peer_at(t), c).start()

    for c in range(GU_PARTS):
        got_gu[c][me] = send_gu[me, pl.ds(c * gu_part, gu_part)]

    s0, s1, s2, s3 = shifts[0], shifts[1], shifts[2], shifts[3]

    def filtered(got, half, done, mean):
        def wide(index):
            return got[lax.rem(index, nodes)].astype(jnp.float32)

        def early(n, total):
            own = wide(n)
            half[n] = (own + wide(n + s0)) + (wide(n + s1) + wide(n + s0 + s1))
            return total + own

        total = lax.fori_loop(0, nodes, early, jnp.zeros(half.shape[1:], jnp.float32), unroll=2)
        mean[...] = total * (1.0 / nodes)

        def late(n, carry):
            value = (half[n] + half[lax.rem(n + s2, nodes)]) + (
                half[lax.rem(n + s3, nodes)] + half[lax.rem(n + s2 + s3, nodes)]
            )
            done[n] = (value * (1.0 / 16.0)).astype(jnp.bfloat16)
            return carry

        lax.fori_loop(0, nodes, late, 0, unroll=2)

    def gu_home(peer, c):
        dst = out_gu.at[me, pl.ds(c * gu_part, gu_part)]
        return exchange(peer, done_gu.at[c, peer], dst, gu_sem, GU_PARTS + c)

    def down_home(peer, c):
        dst = out_down.at[me, pl.ds(c * down_part, down_part)]
        return exchange(peer, done_down.at[c, peer], dst, down_sem, DY_PARTS + c)

    def whole(got, sems, c):
        most = got.at[pl.ds(0, nodes - 1)]
        return exchange((me + 1) % nodes, most, most, sems, c)

    def own_down(c):
        dst = out_down.at[me, pl.ds(c * down_part, down_part)]
        return pltpu.make_async_copy(done_down.at[c, me], dst, keep_down.at[c])

    def own_gu(c):
        dst = out_gu.at[me, pl.ds(c * gu_part, gu_part)]
        return pltpu.make_async_copy(done_gu.at[c, me], dst, keep_gu.at[c])

    for c in range(DY_PARTS):
        whole(got_down[c], down_sem, c).wait_recv()
        filtered(
            got_down[c],
            half_down,
            done_down.at[c],
            mean_down.at[pl.ds(c * down_part, down_part)],
        )

        @pl.loop(1, nodes)
        def _(t):
            down_home(peer_at(t), c).start()

        own_down(c).start()

    for c in range(GU_PARTS):
        whole(got_gu[c], gu_sem, c).wait_recv()
        filtered(
            got_gu[c], half_gu, done_gu.at[c], mean_gu.at[pl.ds(c * gu_part, gu_part)]
        )

        @pl.loop(1, nodes)
        def _(t):
            gu_home(peer_at(t), c).start()

        own_gu(c).start()

    for p in range(len(pieces)):
        to_sibling[p].wait_send()
        to_across[p].wait_send()
        onward[p].wait_send()
    for c in range(DY_PARTS):
        whole(got_down[c], down_sem, c).wait_send()
        whole(got_down[c], down_sem, DY_PARTS + c).wait_send()
        whole(got_down[c], down_sem, DY_PARTS + c).wait_recv()
        own_down(c).wait()
    for c in range(GU_PARTS):
        whole(got_gu[c], gu_sem, c).wait_send()
        whole(got_gu[c], gu_sem, GU_PARTS + c).wait_send()
        whole(got_gu[c], gu_sem, GU_PARTS + c).wait_recv()
        own_gu(c).wait()


def step(param_gu, param_down, tokens, cotangent, routes, plan):
    nodes = lax.axis_size("node")
    experts = lax.axis_size("expert")
    rows, width = tokens.shape
    cols = param_gu.shape[1]
    hid = param_down.shape[0]
    gu_rows = width // nodes
    down_rows = hid // nodes * width // LANES
    dy_cols = width // DY_PARTS
    down_part = 2 * dy_cols // LANES
    pieces = X_PARTS + 1 + DY_PARTS
    named = jnp.sum(jnp.left_shift(jnp.int32(1), routes), axis=1, dtype=jnp.int32)
    code = jnp.broadcast_to(named[None, :], (8, rows))
    shifts = jnp.left_shift(jnp.int32(1), plan)
    everywhere = pl.BlockSpec(memory_space=pl.ANY)
    inside = pl.BlockSpec(memory_space=pltpu.VMEM)
    short, wide = jnp.bfloat16, jnp.float32

    def body(*refs):
        kernel_body(nodes, *refs)

    mixed_gu, mixed_down, mean_gu, mean_down = pl.pallas_call(
        body,
        out_shape=(
            jax.ShapeDtypeStruct((nodes, gu_rows, cols), short),
            jax.ShapeDtypeStruct((nodes, down_rows, LANES), short),
            jax.ShapeDtypeStruct((gu_rows, cols), wide),
            jax.ShapeDtypeStruct((down_rows, LANES), wide),
        ),
        in_specs=[pl.BlockSpec(memory_space=pltpu.SMEM)] + [everywhere] * 5,
        out_specs=(everywhere, everywhere, inside, inside),
        scratch_shapes=[
            pltpu.VMEM((experts * rows, width), short),
            pltpu.VMEM((experts * rows, width), short),
            pltpu.VMEM((width, experts * rows), short),
            pltpu.VMEM((width, cols), wide),
            pltpu.VMEM((hid * width // LANES, LANES), wide),
            pltpu.VMEM((width, cols), short),
            pltpu.VMEM((hid, width), short),
            pltpu.VMEM((experts * rows, cols), wide),
            pltpu.VMEM((experts * rows, hid), wide),
            pltpu.VMEM((hid, experts * rows), short),
            pltpu.VMEM((experts * rows, cols), short),
            pltpu.VMEM((experts, 8, rows), jnp.int32),
            pltpu.VMEM((nodes * down_part, LANES), wide),
            pltpu.VMEM((nodes, gu_rows // GU_PARTS, cols), wide),
            pltpu.VMEM((nodes, down_part, LANES), wide),
            pltpu.VMEM((nodes, gu_rows, cols), short),
            pltpu.VMEM((DY_PARTS, nodes, down_part, LANES), short),
            pltpu.VMEM((GU_PARTS, nodes, gu_rows // GU_PARTS, cols), short),
            pltpu.VMEM((DY_PARTS, nodes, down_part, LANES), short),
            pltpu.SemaphoreType.DMA((1 + pieces,)),
            pltpu.SemaphoreType.DMA((width // LANES,)),
            pltpu.SemaphoreType.DMA((3, pieces)),
            pltpu.SemaphoreType.DMA((3, pieces)),
            pltpu.SemaphoreType.DMA((2, 2 * GU_PARTS)),
            pltpu.SemaphoreType.DMA((2, 2 * DY_PARTS)),
            pltpu.SemaphoreType.DMA((GU_PARTS,)),
            pltpu.SemaphoreType.DMA((DY_PARTS,)),
        ]
        + [pltpu.VMEM((nodes, gu_rows // GU_PARTS, cols), short)] * GU_PARTS
        + [pltpu.VMEM((nodes, down_part, LANES), short)] * DY_PARTS,
        compiler_params=pltpu.CompilerParams(
            collective_id=1, has_side_effects=True, vmem_limit_bytes=56 * 1024 * 1024
        ),
        name="expert_gossip",
    )(shifts, code, tokens, cotangent, param_gu, param_down)

    def unpacked(value):
        parts = value.reshape(-1, DY_PARTS, 2, dy_cols)
        return jnp.swapaxes(parts, 1, 2).reshape(-1, width)

    return (
        mixed_gu.reshape(width, cols),
        unpacked(mixed_down),
        mean_gu,
        unpacked(mean_down[None]),
    )


def solution(mesh):
    both = P(("node", "expert"), None)
    split = P("node", "expert")
    return jax.shard_map(
        step,
        mesh=mesh,
        in_specs=(split, split, both, both, both, P()),
        out_specs=(split, split, split, split),
        check_vma=False,
    )
```

```python
import math

import jax
import jax.numpy as jnp
from jax import lax
from jax.experimental import pallas as pl
from jax.experimental.pallas import tpu as pltpu
from jax.sharding import PartitionSpec as P

MESH = pl.DeviceIdType.MESH
ROUNDS = 4
SHIFTS = 6
X_PARTS = 2
DY_PARTS = 4
GU_PARTS = 4
LANES = 128
TILE = 512
Y_LO, X_SIZE = 2, 4


def kernel_body(
    nodes,
    plan,
    routes,
    tokens,
    cotangent,
    param_gu,
    param_down,
    out_gu,
    out_down,
    mean_gu,
    mean_down,
    x_all,
    dy_all,
    x_turned,
    gu_wide,
    down_wide,
    gu_short,
    down_short,
    both,
    dact,
    act_turned,
    dboth,
    codes,
    stage,
    turned,
    mean_stage,
    half_gu,
    half_down,
    send_gu,
    send_down,
    done_gu,
    done_down,
    home_down,
    last_down,
    enter_sem,
    local_sem,
    block_sem,
    tok_send,
    tok_recv,
    gu_sem,
    down_sem,
    keep_gu,
    keep_down,
    *landing,
):
    got_gu, got_down = landing[:GU_PARTS], landing[GU_PARTS:]
    me = lax.axis_index("node")
    expert = lax.axis_index("expert")
    experts = lax.axis_size("expert")
    plane = Y_LO * X_SIZE
    zs = nodes // plane
    z, y, x = me // plane, (me // X_SIZE) % Y_LO, me % X_SIZE
    sibling = expert + 1 - 2 * (expert % 2)
    across = (expert + 2) % experts
    rows, width = tokens.shape
    hid = param_down.shape[0]
    gu_rows = send_gu.shape[1]
    gu_part = gu_rows // GU_PARTS
    dy_cols = width // DY_PARTS
    blocks = dy_cols // LANES
    down_part = 2 * blocks

    steps = [0] + [d for j in range(1, zs // 2) for d in (j, zs - j)] + [zs // 2]
    z_bases = [((z + d) % zs) * plane for d in steps]

    def in_plane(k):
        return ((y + k // X_SIZE) % Y_LO) * X_SIZE + (x + k % X_SIZE) % X_SIZE

    def each_peer(send):
        @pl.loop(1, plane)
        def _(k):
            send(z_bases[0] + in_plane(k))

        @pl.loop(0, plane)
        def _(k):
            here = in_plane(k)
            for base in z_bases[1:]:
                send(base + here)

    x_cols = width // X_PARTS
    pieces = (
        [(tokens, x_all, pl.ds(c * x_cols, x_cols)) for c in range(X_PARTS)]
        + [(routes, codes, None)]
        + [(cotangent, dy_all, pl.ds(c * dy_cols, dy_cols)) for c in range(DY_PARTS)]
    )

    def source(p):
        src, _, cols = pieces[p]
        return src if cols is None else src.at[:, cols]

    def slot(p, s):
        _, dst, cols = pieces[p]
        if cols is None:
            return dst.at[s]
        return dst.at[pl.ds(s * rows, rows), cols]

    loads = [
        pltpu.make_async_copy(param_gu, gu_wide, local_sem.at[0]),
    ]
    for p in range(len(pieces)):
        loads.append(pltpu.make_async_copy(source(p), slot(p, 0), local_sem.at[1 + p]))
    home = me % plane
    along_z = [((z + d) % zs) * plane + home for d in (1, zs - 1)]
    along_x = [me - x + (x + d) % X_SIZE for d in (1, X_SIZE - 1)]
    along_y = [me - y * X_SIZE + (1 - y) * X_SIZE]
    barrier = pltpu.get_barrier_semaphore()
    for other in (across, sibling):
        pl.semaphore_signal(barrier, inc=1, device_id={"expert": other}, device_id_type=MESH)
    for other in along_z + along_x + along_y:
        pl.semaphore_signal(barrier, inc=1, device_id={"node": other}, device_id_type=MESH)

    for load in loads:
        load.start()

    def down_load(b):
        cols = pl.ds(pl.multiple_of(b * LANES, LANES), LANES)
        dst = down_wide.at[pl.ds(pl.multiple_of(b * hid, hid), hid)]
        return pltpu.make_async_copy(param_down.at[:, cols], dst, block_sem.at[b])

    @pl.loop(0, width // LANES)
    def _(b):
        down_load(b).start()

    pl.semaphore_wait(barrier, 2 + len(along_z + along_x + along_y))

    def token_copy(p, way, src, dst, other):
        return pltpu.make_async_remote_copy(
            src_ref=src,
            dst_ref=dst,
            send_sem=tok_send.at[way, p],
            recv_sem=tok_recv.at[way, p],
            device_id={"expert": other},
            device_id_type=MESH,
        )

    to_sibling = [token_copy(p, 0, source(p), slot(p, 1), sibling) for p in range(len(pieces))]
    to_across = [token_copy(p, 1, source(p), slot(p, 2), across) for p in range(len(pieces))]
    onward = [token_copy(p, 2, slot(p, 2), slot(p, 3), sibling) for p in range(len(pieces))]
    for p in range(len(pieces)):
        to_across[p].start()
        to_sibling[p].start()

    rounds = [along_z] * (zs // 2) + [along_x] * (X_SIZE // 2) + [along_y]
    for r, others in enumerate(rounds):
        for other in others:
            pl.semaphore_signal(
                enter_sem.at[r], inc=1, device_id={"node": other}, device_id_type=MESH
            )
        pl.semaphore_wait(enter_sem.at[r], len(others))

    loads[0].wait()

    @pl.loop(0, width // TILE)
    def _(k):
        span = pl.ds(pl.multiple_of(k * TILE, TILE), TILE)
        gu_short[span, :] = gu_wide[span, :].astype(jnp.bfloat16)

    @pl.loop(0, width // LANES)
    def _(b):
        down_load(b).wait()
        cols = pl.ds(pl.multiple_of(b * LANES, LANES), LANES)
        block = down_wide[pl.ds(pl.multiple_of(b * hid, hid), hid), :]
        down_short[:, cols] = block.astype(jnp.bfloat16)

    both[...] = jnp.zeros_like(both)
    dact[...] = jnp.zeros_like(dact)

    def arrive(p):
        to_across[p].wait_recv()
        onward[p].start()
        loads[1 + p].wait()
        to_sibling[p].wait_recv()
        onward[p].wait_recv()

    for p in range(X_PARTS):
        arrive(p)

        @pl.loop(p * (x_cols // TILE), (p + 1) * (x_cols // TILE))
        def _(k):
            span = pl.ds(pl.multiple_of(k * TILE, TILE), TILE)
            both[...] += jnp.dot(
                x_all[:, span], gu_short[span, :], preferred_element_type=jnp.float32
            )

    arrive(X_PARTS)

    def picked_at(s):
        named = codes[s]
        hit = jnp.where((named[0:1, :] == expert) | (named[1:2, :] == expert), 1, 0)
        return jnp.broadcast_to(hit, (rows, rows)).T != 0

    in_scale = 1.0 / math.sqrt(width)
    hid_scale = 1.0 / math.sqrt(hid)
    first = lax.broadcasted_iota(jnp.int32, (hid, hid), 0)
    second = lax.broadcasted_iota(jnp.int32, (hid, hid), 1)
    wanted = jnp.where(first < hid // 2, 2 * first, 2 * first - (hid - 1))
    order = jnp.where(second == wanted, 1.0, 0.0).astype(jnp.bfloat16)
    for s in range(experts):
        part = pl.ds(s * rows, rows)
        gate = both[part, :hid] * in_scale
        upper = both[part, hid:] * in_scale
        act = jnp.where(picked_at(s), gate * jax.nn.sigmoid(gate) * upper, 0.0)
        act_turned[:, part] = lax.dot_general(
            order,
            act.astype(jnp.bfloat16),
            (((1,), (1,)), ((), ())),
            preferred_element_type=jnp.float32,
        ).astype(jnp.bfloat16)

    @pl.loop(0, width // 256)
    def _(k):
        span = pl.ds(pl.multiple_of(k * 256, 256), 256)
        x_turned[span, :] = x_all[:, span].T

    def exchange(t, src, dst, sems, c):
        return pltpu.make_async_remote_copy(
            src_ref=src,
            dst_ref=dst,
            send_sem=sems.at[0, c],
            recv_sem=sems.at[1, c],
            device_id={"node": t},
            device_id_type=MESH,
        )

    def gu_out(peer, c):
        return exchange(
            peer, send_gu.at[peer, pl.ds(c * gu_part, gu_part)], got_gu[c].at[me], gu_sem, c
        )

    def down_out(peer, c):
        return exchange(peer, send_down.at[c, peer], got_down[c].at[me], down_sem, c)

    for c in range(DY_PARTS):
        arrive(X_PARTS + 1 + c)

        @pl.loop(0, dy_cols // TILE)
        def _(k):
            at = pl.multiple_of(c * dy_cols + k * TILE, TILE)
            span = pl.ds(at, TILE)
            dact[...] += lax.dot_general(
                dy_all[:, span],
                down_short[:, span],
                (((1,), (1,)), ((), ())),
                preferred_element_type=jnp.float32,
            )
            grad = jnp.dot(act_turned[...], dy_all[:, span], preferred_element_type=jnp.float32)
            grad = grad * (0.5 * hid_scale)
            for r in range(2):
                for i in range(TILE // LANES):
                    block = c * blocks + k * (TILE // LANES) + i
                    old = down_wide[pl.ds(block * hid + r, nodes, stride=2), :]
                    new = old - grad[r * nodes : (r + 1) * nodes, i * LANES : (i + 1) * LANES]
                    row = r * blocks + k * (TILE // LANES) + i
                    stage[pl.ds(row, nodes, stride=down_part), :] = new

        @pl.loop(0, nodes)
        def _(n):
            span = pl.ds(pl.multiple_of(n * down_part, down_part), down_part)
            send_down[c, n] = stage[span, :].astype(jnp.bfloat16)

        each_peer(lambda peer: down_out(peer, c).start())

        got_down[c][me] = send_down[c, me]

    for s in range(experts):
        part = pl.ds(s * rows, rows)
        gate = both[part, :hid] * in_scale
        upper = both[part, hid:] * in_scale
        sigma = jax.nn.sigmoid(gate)
        da = dact[part, :] * hid_scale
        picked = picked_at(s)
        dgate = da * upper * sigma * (1.0 + gate * (1.0 - sigma))
        dupper = da * gate * sigma
        dboth[part, :hid] = jnp.where(picked, dgate, 0.0).astype(jnp.bfloat16)
        dboth[part, hid:] = jnp.where(picked, dupper, 0.0).astype(jnp.bfloat16)

    @pl.loop(0, zs)
    def _(j):
        zt = (z + (j % 2) * ((j + 1) // 2) + (1 - j % 2) * (zs - j // 2)) % zs
        at = pl.multiple_of(zt * (plane * gu_rows), plane * gu_rows)
        span = pl.ds(at, plane * gu_rows)
        grad = jnp.dot(x_turned[span, :], dboth[...], preferred_element_type=jnp.float32)
        new = gu_wide[span, :] - grad * (0.5 * in_scale)
        send_gu[pl.ds(zt * plane, plane)] = new.astype(jnp.bfloat16).reshape(
            plane, gu_rows, new.shape[1]
        )
        for k in range(plane):
            peer = zt * plane + in_plane(k)
            if k == 0:

                @pl.when(j > 0)
                def _():
                    gu_out(peer, 0).start()

            else:
                gu_out(peer, 0).start()

    for c in range(1, GU_PARTS):

        each_peer(lambda peer: gu_out(peer, c).start())

    for c in range(GU_PARTS):
        got_gu[c][me] = send_gu[me, pl.ds(c * gu_part, gu_part)]

    def shift_at(i):
        exponent, shift = plan[i], jnp.int32(1)
        for e in range(1, SHIFTS):
            shift = jnp.where(exponent == e, jnp.int32(1 << e), shift)
        return shift

    s0, s1, s2, s3 = (shift_at(i) for i in range(ROUNDS))

    def filtered(got, half, done, mean):
        def wide(index):
            return got[lax.rem(index, nodes)].astype(jnp.float32)

        def early(n, total):
            own = wide(n)
            half[n] = (own + wide(n + s0)) + (wide(n + s1) + wide(n + s0 + s1))
            return total + own

        total = lax.fori_loop(0, nodes, early, jnp.zeros(half.shape[1:], jnp.float32), unroll=2)
        mean[...] = total * (1.0 / nodes)

        def late(n, carry):
            value = (half[n] + half[lax.rem(n + s2, nodes)]) + (
                half[lax.rem(n + s3, nodes)] + half[lax.rem(n + s2 + s3, nodes)]
            )
            done[n] = (value * (1.0 / 16.0)).astype(jnp.bfloat16)
            return carry

        lax.fori_loop(0, nodes, late, 0, unroll=2)

    def gu_home(peer, c):
        dst = out_gu.at[me, pl.ds(c * gu_part, gu_part)]
        return exchange(peer, done_gu.at[c, peer], dst, gu_sem, GU_PARTS + c)

    def down_home(peer, c):
        return exchange(
            peer, done_down.at[c, peer], home_down.at[c, me], down_sem, DY_PARTS + c
        )

    def whole(got, sems, c):
        most = got.at[pl.ds(0, nodes - 1)]
        return exchange((me + 1) % nodes, most, most, sems, c)

    def put_down(c):
        cols = pl.ds(c * dy_cols, dy_cols)
        return pltpu.make_async_copy(last_down.at[c], out_down.at[:, cols], keep_down.at[c])

    def own_gu(c):
        dst = out_gu.at[me, pl.ds(c * gu_part, gu_part)]
        return pltpu.make_async_copy(done_gu.at[c, me], dst, keep_gu.at[c])

    for c in range(DY_PARTS):
        whole(got_down[c], down_sem, c).wait_recv()
        filtered(
            got_down[c],
            half_down,
            done_down.at[c],
            mean_stage,
        )
        for r in range(2):
            for i in range(blocks):
                at = c * dy_cols + i * LANES
                mean_down[r : r + 1, at : at + LANES] = mean_stage[
                    r * blocks + i : r * blocks + i + 1, :
                ]

        each_peer(lambda peer: down_home(peer, c).start())

        home_down[c, me] = done_down[c, me]

    for c in range(GU_PARTS):
        whole(got_gu[c], gu_sem, c).wait_recv()
        filtered(
            got_gu[c], half_gu, done_gu.at[c], mean_gu.at[pl.ds(c * gu_part, gu_part)]
        )

        each_peer(lambda peer: gu_home(peer, c).start())

        own_gu(c).start()

    for c in range(DY_PARTS):
        whole(got_down[c], down_sem, DY_PARTS + c).wait_recv()

        @pl.loop(0, nodes)
        def _(n):
            span = pl.ds(pl.multiple_of(n * down_part, down_part), down_part)
            stage[span, :] = home_down[c, n].astype(jnp.float32)

        for i in range(blocks):
            for r in range(2):
                row = r * blocks + i
                turned[pl.ds(i * hid + r, nodes, stride=2), :] = stage[
                    pl.ds(row, nodes, stride=down_part), :
                ]
            last_down[c, :, i * LANES : (i + 1) * LANES] = turned[
                i * hid : (i + 1) * hid, :
            ].astype(jnp.bfloat16)
        put_down(c).start()

    for p in range(len(pieces)):
        to_sibling[p].wait_send()
        to_across[p].wait_send()
        onward[p].wait_send()
    for c in range(DY_PARTS):
        whole(got_down[c], down_sem, c).wait_send()
        whole(got_down[c], down_sem, DY_PARTS + c).wait_send()
        put_down(c).wait()
    for c in range(GU_PARTS):
        whole(got_gu[c], gu_sem, c).wait_send()
        whole(got_gu[c], gu_sem, GU_PARTS + c).wait_send()
        whole(got_gu[c], gu_sem, GU_PARTS + c).wait_recv()
        own_gu(c).wait()


def step(param_gu, param_down, tokens, cotangent, routes, plan):
    nodes = lax.axis_size("node")
    experts = lax.axis_size("expert")
    rows, width = tokens.shape
    cols = param_gu.shape[1]
    hid = param_down.shape[0]
    gu_rows = width // nodes
    dy_cols = width // DY_PARTS
    down_part = 2 * dy_cols // LANES
    pieces = X_PARTS + 1 + DY_PARTS
    everywhere = pl.BlockSpec(memory_space=pl.ANY)
    inside = pl.BlockSpec(memory_space=pltpu.VMEM)
    short, wide = jnp.bfloat16, jnp.float32

    def body(*refs):
        kernel_body(nodes, *refs)

    mixed_gu, mixed_down, mean_gu, mean_down = pl.pallas_call(
        body,
        out_shape=(
            jax.ShapeDtypeStruct((nodes, gu_rows, cols), short),
            jax.ShapeDtypeStruct((hid, width), short),
            jax.ShapeDtypeStruct((gu_rows, cols), wide),
            jax.ShapeDtypeStruct((hid // nodes, width), wide),
        ),
        in_specs=[pl.BlockSpec(memory_space=pltpu.SMEM)] + [everywhere] * 5,
        out_specs=(everywhere, everywhere, inside, inside),
        scratch_shapes=[
            pltpu.VMEM((experts * rows, width), short),
            pltpu.VMEM((experts * rows, width), short),
            pltpu.VMEM((width, experts * rows), short),
            pltpu.VMEM((width, cols), wide),
            pltpu.VMEM((hid * width // LANES, LANES), wide),
            pltpu.VMEM((width, cols), short),
            pltpu.VMEM((hid, width), short),
            pltpu.VMEM((experts * rows, cols), wide),
            pltpu.VMEM((experts * rows, hid), wide),
            pltpu.VMEM((hid, experts * rows), short),
            pltpu.VMEM((experts * rows, cols), short),
            pltpu.VMEM((experts, 2, rows), jnp.int32),
            pltpu.VMEM((nodes * down_part, LANES), wide),
            pltpu.VMEM((nodes * down_part, LANES), wide),
            pltpu.VMEM((down_part, LANES), wide),
            pltpu.VMEM((nodes, gu_rows // GU_PARTS, cols), wide),
            pltpu.VMEM((nodes, down_part, LANES), wide),
            pltpu.VMEM((nodes, gu_rows, cols), short),
            pltpu.VMEM((DY_PARTS, nodes, down_part, LANES), short),
            pltpu.VMEM((GU_PARTS, nodes, gu_rows // GU_PARTS, cols), short),
            pltpu.VMEM((DY_PARTS, nodes, down_part, LANES), short),
            pltpu.VMEM((DY_PARTS, nodes, down_part, LANES), short),
            pltpu.VMEM((DY_PARTS, hid, dy_cols), short),
            pltpu.SemaphoreType.REGULAR((nodes // (Y_LO * X_SIZE) // 2 + X_SIZE // 2 + 1,)),
            pltpu.SemaphoreType.DMA((1 + pieces,)),
            pltpu.SemaphoreType.DMA((width // LANES,)),
            pltpu.SemaphoreType.DMA((3, pieces)),
            pltpu.SemaphoreType.DMA((3, pieces)),
            pltpu.SemaphoreType.DMA((2, 2 * GU_PARTS)),
            pltpu.SemaphoreType.DMA((2, 2 * DY_PARTS)),
            pltpu.SemaphoreType.DMA((GU_PARTS,)),
            pltpu.SemaphoreType.DMA((DY_PARTS,)),
        ]
        + [pltpu.VMEM((nodes, gu_rows // GU_PARTS, cols), short)] * GU_PARTS
        + [pltpu.VMEM((nodes, down_part, LANES), short)] * DY_PARTS,
        compiler_params=pltpu.CompilerParams(
            collective_id=1, has_side_effects=True, vmem_limit_bytes=56 * 1024 * 1024
        ),
        name="expert_gossip",
    )(plan, routes.T, tokens, cotangent, param_gu, param_down)

    return mixed_gu.reshape(width, cols), mixed_down, mean_gu, mean_down


def solution(mesh):
    both = P(("node", "expert"), None)
    split = P("node", "expert")
    return jax.shard_map(
        step,
        mesh=mesh,
        in_specs=(split, split, both, both, both, P()),
        out_specs=(split, split, split, split),
        check_vma=False,
    )
```

```python
import math

import jax
import jax.numpy as jnp
from jax import lax
from jax.experimental import pallas as pl
from jax.experimental.pallas import tpu as pltpu
from jax.sharding import PartitionSpec as P

MESH = pl.DeviceIdType.MESH
ROUNDS = 4
SHIFTS = 6
X_PARTS = 2
DY_BLOCKS = (4, 4, 8, 8, 8)
DY_PARTS = len(DY_BLOCKS)
GU_PARTS = 4
LANES = 128
TILE = 512
Y_LO, X_SIZE = 2, 4


def kernel_body(
    nodes,
    plan,
    routes,
    tokens,
    cotangent,
    param_gu,
    param_down,
    out_gu,
    out_down,
    mean_gu,
    mean_down,
    x_all,
    dy_all,
    x_turned,
    gu_wide,
    down_wide,
    gu_short,
    down_short,
    both,
    dact,
    act_turned,
    dboth,
    codes,
    stage,
    turned,
    mean_stage,
    mean_rows,
    mean_slab,
    mean_sem,
    half_gu,
    half_down,
    send_gu,
    done_gu,
    enter_sem,
    local_sem,
    block_sem,
    tok_send,
    tok_recv,
    gu_sem,
    down_sem,
    keep_gu,
    keep_down,
    *landing,
):
    got_gu, downs = landing[:GU_PARTS], landing[GU_PARTS:]
    send_down, got_down, done_down, home_down, last_down = (
        downs[i * DY_PARTS : (i + 1) * DY_PARTS] for i in range(5)
    )
    me = lax.axis_index("node")
    expert = lax.axis_index("expert")
    experts = lax.axis_size("expert")
    plane = Y_LO * X_SIZE
    zs = nodes // plane
    z, y, x = me // plane, (me // X_SIZE) % Y_LO, me % X_SIZE
    sibling = expert + 1 - 2 * (expert % 2)
    across = (expert + 2) % experts
    rows, width = tokens.shape
    hid = param_down.shape[0]
    gu_rows = send_gu.shape[1]
    gu_part = gu_rows // GU_PARTS
    starts = [sum(DY_BLOCKS[:c]) for c in range(DY_PARTS)]

    steps = [0] + [d for j in range(1, zs // 2) for d in (j, zs - j)] + [zs // 2]
    z_bases = [((z + d) % zs) * plane for d in steps]

    def in_plane(k):
        return ((y + k // X_SIZE) % Y_LO) * X_SIZE + (x + k % X_SIZE) % X_SIZE

    def each_peer(send):
        @pl.loop(1, plane)
        def _(k):
            send(z_bases[0] + in_plane(k))

        @pl.loop(0, plane)
        def _(k):
            here = in_plane(k)
            for base in z_bases[1:]:
                send(base + here)

    x_cols = width // X_PARTS
    pieces = (
        [(routes, codes, None)]
        + [(tokens, x_all, pl.ds(c * x_cols, x_cols)) for c in range(X_PARTS)]
        + [
            (cotangent, dy_all, pl.ds(starts[c] * LANES, DY_BLOCKS[c] * LANES))
            for c in range(DY_PARTS)
        ]
    )

    def source(p):
        src, _, cols = pieces[p]
        return src if cols is None else src.at[:, cols]

    def slot(p, s):
        _, dst, cols = pieces[p]
        if cols is None:
            return dst.at[s]
        return dst.at[pl.ds(s * rows, rows), cols]

    loads = [
        pltpu.make_async_copy(source(p), slot(p, 0), local_sem.at[p]) for p in range(len(pieces))
    ]
    loads.append(pltpu.make_async_copy(param_gu, gu_wide, local_sem.at[len(pieces)]))
    home = me % plane
    along_z = [((z + d) % zs) * plane + home for d in (1, zs - 1)]
    along_x = [me - x + (x + d) % X_SIZE for d in (1, X_SIZE - 1)]
    along_y = [me - y * X_SIZE + (1 - y) * X_SIZE]
    barrier = pltpu.get_barrier_semaphore()
    for other in (across, sibling):
        pl.semaphore_signal(barrier, inc=1, device_id={"expert": other}, device_id_type=MESH)
    for other in along_z + along_x + along_y:
        pl.semaphore_signal(barrier, inc=1, device_id={"node": other}, device_id_type=MESH)

    for load in loads:
        load.start()

    def down_load(b):
        cols = pl.ds(pl.multiple_of(b * LANES, LANES), LANES)
        dst = down_wide.at[pl.ds(pl.multiple_of(b * hid, hid), hid)]
        return pltpu.make_async_copy(param_down.at[:, cols], dst, block_sem.at[b])

    @pl.loop(0, width // LANES)
    def _(b):
        down_load(b).start()

    pl.semaphore_wait(barrier, 2 + len(along_z + along_x + along_y))

    def token_copy(p, way, src, dst, other):
        return pltpu.make_async_remote_copy(
            src_ref=src,
            dst_ref=dst,
            send_sem=tok_send.at[way, p],
            recv_sem=tok_recv.at[way, p],
            device_id={"expert": other},
            device_id_type=MESH,
        )

    to_sibling = [token_copy(p, 0, slot(p, 0), slot(p, 1), sibling) for p in range(len(pieces))]
    to_across = [token_copy(p, 1, slot(p, 0), slot(p, 2), across) for p in range(len(pieces))]
    onward = [token_copy(p, 2, slot(p, 2), slot(p, 3), sibling) for p in range(len(pieces))]
    for p in range(len(pieces)):
        loads[p].wait()
        to_across[p].start()
        to_sibling[p].start()

    rounds = [along_z] * (zs // 2) + [along_x] * (X_SIZE // 2) + [along_y]
    for r, others in enumerate(rounds):
        for other in others:
            pl.semaphore_signal(
                enter_sem.at[r], inc=1, device_id={"node": other}, device_id_type=MESH
            )
        pl.semaphore_wait(enter_sem.at[r], len(others))

    loads[-1].wait()

    @pl.loop(0, width // TILE)
    def _(k):
        span = pl.ds(pl.multiple_of(k * TILE, TILE), TILE)
        gu_short[span, :] = gu_wide[span, :].astype(jnp.bfloat16)

    @pl.loop(0, width // LANES)
    def _(b):
        down_load(b).wait()
        cols = pl.ds(pl.multiple_of(b * LANES, LANES), LANES)
        block = down_wide[pl.ds(pl.multiple_of(b * hid, hid), hid), :]
        down_short[:, cols] = block.astype(jnp.bfloat16)

    both[...] = jnp.zeros_like(both)
    dact[...] = jnp.zeros_like(dact)

    def arrive(p):
        to_across[p].wait_recv()
        onward[p].start()
        to_sibling[p].wait_recv()
        onward[p].wait_recv()

    arrive(0)
    for p in range(X_PARTS):
        arrive(1 + p)

        @pl.loop(p * (x_cols // TILE), (p + 1) * (x_cols // TILE))
        def _(k):
            span = pl.ds(pl.multiple_of(k * TILE, TILE), TILE)
            both[...] += jnp.dot(
                x_all[:, span], gu_short[span, :], preferred_element_type=jnp.float32
            )

    def picked_at(s):
        named = codes[s]
        hit = jnp.where((named[0:1, :] == expert) | (named[1:2, :] == expert), 1, 0)
        return jnp.broadcast_to(hit, (rows, rows)).T != 0

    in_scale = 1.0 / math.sqrt(width)
    hid_scale = 1.0 / math.sqrt(hid)
    first = lax.broadcasted_iota(jnp.int32, (hid, hid), 0)
    second = lax.broadcasted_iota(jnp.int32, (hid, hid), 1)
    wanted = jnp.where(first < hid // 2, 2 * first, 2 * first - (hid - 1))
    order = jnp.where(second == wanted, 1.0, 0.0).astype(jnp.bfloat16)
    for s in range(experts):
        part = pl.ds(s * rows, rows)
        gate = both[part, :hid] * in_scale
        upper = both[part, hid:] * in_scale
        act = jnp.where(picked_at(s), gate * jax.nn.sigmoid(gate) * upper, 0.0)
        act_turned[:, part] = lax.dot_general(
            order,
            act.astype(jnp.bfloat16),
            (((1,), (1,)), ((), ())),
            preferred_element_type=jnp.float32,
        ).astype(jnp.bfloat16)

    @pl.loop(0, width // 256)
    def _(k):
        span = pl.ds(pl.multiple_of(k * 256, 256), 256)
        x_turned[span, :] = x_all[:, span].T

    def exchange(t, src, dst, sems, c):
        return pltpu.make_async_remote_copy(
            src_ref=src,
            dst_ref=dst,
            send_sem=sems.at[0, c],
            recv_sem=sems.at[1, c],
            device_id={"node": t},
            device_id_type=MESH,
        )

    def gu_out(peer, c):
        return exchange(
            peer, send_gu.at[peer, pl.ds(c * gu_part, gu_part)], got_gu[c].at[me], gu_sem, c
        )

    def down_out(peer, c):
        return exchange(peer, send_down[c].at[peer], got_down[c].at[me], down_sem, c)

    for c in range(DY_PARTS):
        arrive(1 + X_PARTS + c)
        blocks = DY_BLOCKS[c]
        down_part = 2 * blocks

        @pl.loop(0, blocks * LANES // TILE)
        def _(k):
            at = pl.multiple_of(starts[c] * LANES + k * TILE, TILE)
            span = pl.ds(at, TILE)
            dact[...] += lax.dot_general(
                dy_all[:, span],
                down_short[:, span],
                (((1,), (1,)), ((), ())),
                preferred_element_type=jnp.float32,
            )
            grad = jnp.dot(act_turned[...], dy_all[:, span], preferred_element_type=jnp.float32)
            grad = grad * (0.5 * hid_scale)
            for r in range(2):
                for i in range(TILE // LANES):
                    block = starts[c] + k * (TILE // LANES) + i
                    old = down_wide[pl.ds(block * hid + r, nodes, stride=2), :]
                    new = old - grad[r * nodes : (r + 1) * nodes, i * LANES : (i + 1) * LANES]
                    row = r * blocks + k * (TILE // LANES) + i
                    stage[pl.ds(row, nodes, stride=down_part), :] = new

        @pl.loop(0, nodes)
        def _(n):
            span = pl.ds(pl.multiple_of(n * down_part, down_part), down_part)
            send_down[c][n] = stage[span, :].astype(jnp.bfloat16)

        each_peer(lambda peer: down_out(peer, c).start())

        got_down[c][me] = send_down[c][me]

    for s in range(experts):
        part = pl.ds(s * rows, rows)
        gate = both[part, :hid] * in_scale
        upper = both[part, hid:] * in_scale
        sigma = jax.nn.sigmoid(gate)
        da = dact[part, :] * hid_scale
        picked = picked_at(s)
        dgate = da * upper * sigma * (1.0 + gate * (1.0 - sigma))
        dupper = da * gate * sigma
        dboth[part, :hid] = jnp.where(picked, dgate, 0.0).astype(jnp.bfloat16)
        dboth[part, hid:] = jnp.where(picked, dupper, 0.0).astype(jnp.bfloat16)

    @pl.loop(0, zs)
    def _(j):
        zt = (z + (j % 2) * ((j + 1) // 2) + (1 - j % 2) * (zs - j // 2)) % zs
        at = pl.multiple_of(zt * (plane * gu_rows), plane * gu_rows)
        span = pl.ds(at, plane * gu_rows)
        grad = jnp.dot(x_turned[span, :], dboth[...], preferred_element_type=jnp.float32)
        new = gu_wide[span, :] - grad * (0.5 * in_scale)
        send_gu[pl.ds(zt * plane, plane)] = new.astype(jnp.bfloat16).reshape(
            plane, gu_rows, new.shape[1]
        )
        for k in range(plane):
            peer = zt * plane + in_plane(k)
            if k == 0:

                @pl.when(j > 0)
                def _():
                    gu_out(peer, 0).start()

            else:
                gu_out(peer, 0).start()

    for c in range(1, GU_PARTS):

        each_peer(lambda peer: gu_out(peer, c).start())

    for c in range(GU_PARTS):
        got_gu[c][me] = send_gu[me, pl.ds(c * gu_part, gu_part)]

    def shift_at(i):
        exponent, shift = plan[i], jnp.int32(1)
        for e in range(1, SHIFTS):
            shift = jnp.where(exponent == e, jnp.int32(1 << e), shift)
        return shift

    s0, s1, s2, s3 = (shift_at(i) for i in range(ROUNDS))

    def filtered(got, half, done, mean):
        def wide(index):
            return got[lax.rem(index, nodes)].astype(jnp.float32)

        def early(n, total):
            own = wide(n)
            half[n] = (own + wide(n + s0)) + (wide(n + s1) + wide(n + s0 + s1))
            return total + own

        total = lax.fori_loop(0, nodes, early, jnp.zeros(half.shape[1:], jnp.float32), unroll=2)
        mean[...] = total * (1.0 / nodes)

        def late(n, carry):
            value = (half[n] + half[lax.rem(n + s2, nodes)]) + (
                half[lax.rem(n + s3, nodes)] + half[lax.rem(n + s2 + s3, nodes)]
            )
            done[n] = (value * (1.0 / 16.0)).astype(jnp.bfloat16)
            return carry

        lax.fori_loop(0, nodes, late, 0, unroll=2)

    def gu_home(peer, c):
        dst = out_gu.at[me, pl.ds(c * gu_part, gu_part)]
        return exchange(peer, done_gu.at[c, peer], dst, gu_sem, GU_PARTS + c)

    def down_home(peer, c):
        return exchange(
            peer, done_down[c].at[peer], home_down[c].at[me], down_sem, DY_PARTS + c
        )

    def whole(got, sems, c):
        most = got.at[pl.ds(0, nodes - 1)]
        return exchange((me + 1) % nodes, most, most, sems, c)

    def put_down(c):
        cols = pl.ds(starts[c] * LANES, DY_BLOCKS[c] * LANES)
        return pltpu.make_async_copy(last_down[c], out_down.at[:, cols], keep_down.at[c])

    def own_gu(c):
        dst = out_gu.at[me, pl.ds(c * gu_part, gu_part)]
        return pltpu.make_async_copy(done_gu.at[c, me], dst, keep_gu.at[c])

    for c in range(DY_PARTS):
        whole(got_down[c], down_sem, c).wait_recv()
        blocks = DY_BLOCKS[c]
        filtered(
            got_down[c],
            half_down.at[:, pl.ds(0, 2 * blocks)],
            done_down[c],
            mean_stage.at[pl.ds(0, 2 * blocks)],
        )
        for r in range(2):
            for i in range(blocks):
                at = (starts[c] + i) * LANES
                mean_rows[r : r + 1, at : at + LANES] = mean_stage[
                    r * blocks + i : r * blocks + i + 1, :
                ]

        each_peer(lambda peer: down_home(peer, c).start())

        home_down[c][me] = done_down[c][me]

    for c in range(GU_PARTS):
        whole(got_gu[c], gu_sem, c).wait_recv()
        filtered(
            got_gu[c], half_gu, done_gu.at[c], mean_slab.at[pl.ds(c * gu_part, gu_part)]
        )

        each_peer(lambda peer: gu_home(peer, c).start())

        own_gu(c).start()

    means = [
        pltpu.make_async_copy(mean_slab, mean_gu, mean_sem.at[0]),
        pltpu.make_async_copy(mean_rows, mean_down, mean_sem.at[1]),
    ]
    for copy in means:
        copy.start()

    for c in range(DY_PARTS):
        whole(got_down[c], down_sem, DY_PARTS + c).wait_recv()
        blocks = DY_BLOCKS[c]
        down_part = 2 * blocks

        @pl.loop(0, nodes)
        def _(n):
            span = pl.ds(pl.multiple_of(n * down_part, down_part), down_part)
            stage[span, :] = home_down[c][n].astype(jnp.float32)

        for i in range(blocks):
            for r in range(2):
                row = r * blocks + i
                turned[pl.ds(i * hid + r, nodes, stride=2), :] = stage[
                    pl.ds(row, nodes, stride=down_part), :
                ]
            last_down[c][:, i * LANES : (i + 1) * LANES] = turned[
                i * hid : (i + 1) * hid, :
            ].astype(jnp.bfloat16)
        put_down(c).start()

    for copy in means:
        copy.wait()
    for p in range(len(pieces)):
        to_sibling[p].wait_send()
        to_across[p].wait_send()
        onward[p].wait_send()
    for c in range(DY_PARTS):
        whole(got_down[c], down_sem, c).wait_send()
        whole(got_down[c], down_sem, DY_PARTS + c).wait_send()
        put_down(c).wait()
    for c in range(GU_PARTS):
        whole(got_gu[c], gu_sem, c).wait_send()
        whole(got_gu[c], gu_sem, GU_PARTS + c).wait_send()
        whole(got_gu[c], gu_sem, GU_PARTS + c).wait_recv()
        own_gu(c).wait()


def step(param_gu, param_down, tokens, cotangent, routes, plan):
    nodes = lax.axis_size("node")
    experts = lax.axis_size("expert")
    rows, width = tokens.shape
    cols = param_gu.shape[1]
    hid = param_down.shape[0]
    gu_rows = width // nodes
    down_part = 2 * max(DY_BLOCKS)
    pieces = X_PARTS + 1 + DY_PARTS
    everywhere = pl.BlockSpec(memory_space=pl.ANY)
    outside = pl.BlockSpec(memory_space=pltpu.HBM)
    short, wide = jnp.bfloat16, jnp.float32

    def body(*refs):
        kernel_body(nodes, *refs)

    held = [
        pltpu.with_memory_space_constraint(a, pltpu.HBM)
        for a in (routes.T, tokens, cotangent, param_gu, param_down)
    ]
    mixed_gu, mixed_down, mean_gu, mean_down = pl.pallas_call(
        body,
        out_shape=(
            jax.ShapeDtypeStruct((nodes, gu_rows, cols), short),
            jax.ShapeDtypeStruct((hid, width), short),
            jax.ShapeDtypeStruct((gu_rows, cols), wide),
            jax.ShapeDtypeStruct((hid // nodes, width), wide),
        ),
        in_specs=[pl.BlockSpec(memory_space=pltpu.SMEM)] + [outside] * 5,
        out_specs=(everywhere,) * 4,
        scratch_shapes=[
            pltpu.VMEM((experts * rows, width), short),
            pltpu.VMEM((experts * rows, width), short),
            pltpu.VMEM((width, experts * rows), short),
            pltpu.VMEM((width, cols), wide),
            pltpu.VMEM((hid * width // LANES, LANES), wide),
            pltpu.VMEM((width, cols), short),
            pltpu.VMEM((hid, width), short),
            pltpu.VMEM((experts * rows, cols), wide),
            pltpu.VMEM((experts * rows, hid), wide),
            pltpu.VMEM((hid, experts * rows), short),
            pltpu.VMEM((experts * rows, cols), short),
            pltpu.VMEM((experts, 2, rows), jnp.int32),
            pltpu.VMEM((nodes * down_part, LANES), wide),
            pltpu.VMEM((nodes * down_part, LANES), wide),
            pltpu.VMEM((down_part, LANES), wide),
            pltpu.VMEM((hid // nodes, width), wide),
            pltpu.VMEM((gu_rows, cols), wide),
            pltpu.SemaphoreType.DMA((2,)),
            pltpu.VMEM((nodes, gu_rows // GU_PARTS, cols), wide),
            pltpu.VMEM((nodes, down_part, LANES), wide),
            pltpu.VMEM((nodes, gu_rows, cols), short),
            pltpu.VMEM((GU_PARTS, nodes, gu_rows // GU_PARTS, cols), short),
            pltpu.SemaphoreType.REGULAR((nodes // (Y_LO * X_SIZE) // 2 + X_SIZE // 2 + 1,)),
            pltpu.SemaphoreType.DMA((1 + pieces,)),
            pltpu.SemaphoreType.DMA((width // LANES,)),
            pltpu.SemaphoreType.DMA((3, pieces)),
            pltpu.SemaphoreType.DMA((3, pieces)),
            pltpu.SemaphoreType.DMA((2, 2 * GU_PARTS)),
            pltpu.SemaphoreType.DMA((2, 2 * DY_PARTS)),
            pltpu.SemaphoreType.DMA((GU_PARTS,)),
            pltpu.SemaphoreType.DMA((DY_PARTS,)),
        ]
        + [pltpu.VMEM((nodes, gu_rows // GU_PARTS, cols), short)] * GU_PARTS
        + [pltpu.VMEM((nodes, 2 * b, LANES), short) for b in DY_BLOCKS] * 4
        + [pltpu.VMEM((hid, b * LANES), short) for b in DY_BLOCKS],
        compiler_params=pltpu.CompilerParams(
            collective_id=1, has_side_effects=True, vmem_limit_bytes=48 * 1024 * 1024
        ),
        name="expert_gossip",
    )(plan, *held)

    return mixed_gu.reshape(width, cols), mixed_down, mean_gu, mean_down


def solution(mesh):
    both = P(("node", "expert"), None)
    split = P("node", "expert")
    return jax.shard_map(
        step,
        mesh=mesh,
        in_specs=(split, split, both, both, both, P()),
        out_specs=(split, split, split, split),
        check_vma=False,
    )
```

```python
import math

import jax
import jax.numpy as jnp
from jax import lax
from jax.experimental import pallas as pl
from jax.experimental.pallas import tpu as pltpu
from jax.sharding import PartitionSpec as P

MESH = pl.DeviceIdType.MESH
ROUNDS = 4
SHIFTS = 6
X_PARTS = 4
DY_BLOCKS = (4, 4, 8, 8, 8)
DY_PARTS = len(DY_BLOCKS)
GU_PARTS = 4
LANES = 128
TILE = 512
Y_LO, X_SIZE = 2, 4


def kernel_body(
    nodes,
    plan,
    routes,
    tokens,
    cotangent,
    param_gu,
    param_down,
    out_gu,
    out_down,
    mean_gu,
    mean_down,
    x_all,
    dy_all,
    x_turned,
    gu_wide,
    down_wide,
    gu_short,
    down_short,
    both,
    dact,
    act_turned,
    dboth,
    codes,
    stage,
    turned,
    mean_stage,
    mean_rows,
    mean_slab,
    mean_sem,
    half_gu,
    half_down,
    send_gu,
    done_gu,
    enter_sem,
    local_sem,
    block_sem,
    tok_send,
    tok_recv,
    gu_sem,
    down_sem,
    relay_sem,
    over_sem,
    keep_gu,
    keep_down,
    *landing,
):
    got_gu, downs = landing[:GU_PARTS], landing[GU_PARTS:]
    send_down, got_down, done_down, home_down, relay_down, last_down = (
        downs[i * DY_PARTS : (i + 1) * DY_PARTS] for i in range(6)
    )
    me = lax.axis_index("node")
    expert = lax.axis_index("expert")
    experts = lax.axis_size("expert")
    plane = Y_LO * X_SIZE
    zs = nodes // plane
    z, y, x = me // plane, (me // X_SIZE) % Y_LO, me % X_SIZE
    sibling = expert + 1 - 2 * (expert % 2)
    across = (expert + 2) % experts
    rows, width = tokens.shape
    hid = param_down.shape[0]
    gu_rows = send_gu.shape[1]
    gu_part = gu_rows // GU_PARTS
    starts = [sum(DY_BLOCKS[:c]) for c in range(DY_PARTS)]

    steps = [0] + [d for j in range(1, zs // 2) for d in (j, zs - j)] + [zs // 2]
    z_bases = [((z + d) % zs) * plane for d in steps]

    def in_plane(k):
        return ((y + k // X_SIZE) % Y_LO) * X_SIZE + (x + k % X_SIZE) % X_SIZE

    def each_peer(send):
        @pl.loop(1, plane)
        def _(k):
            send(z_bases[0] + in_plane(k))

        @pl.loop(0, plane)
        def _(k):
            here = in_plane(k)
            for base in z_bases[1:]:
                send(base + here)

    x_cols = width // X_PARTS
    pieces = (
        [(routes, codes, None)]
        + [(tokens, x_all, pl.ds(c * x_cols, x_cols)) for c in range(X_PARTS)]
        + [
            (cotangent, dy_all, pl.ds(starts[c] * LANES, DY_BLOCKS[c] * LANES))
            for c in range(DY_PARTS)
        ]
    )

    def source(p):
        src, _, cols = pieces[p]
        return src if cols is None else src.at[:, cols]

    def slot(p, s):
        _, dst, cols = pieces[p]
        if cols is None:
            return dst.at[s]
        return dst.at[pl.ds(s * rows, rows), cols]

    loads = [
        pltpu.make_async_copy(source(p), slot(p, 0), local_sem.at[p]) for p in range(len(pieces))
    ]
    loads.append(pltpu.make_async_copy(param_gu, gu_wide, local_sem.at[len(pieces)]))
    home = me % plane
    along_z = [((z + d) % zs) * plane + home for d in (1, zs - 1)]
    along_x = [me - x + (x + d) % X_SIZE for d in (1, X_SIZE - 1)]
    along_y = [me - y * X_SIZE + (1 - y) * X_SIZE]
    barrier = pltpu.get_barrier_semaphore()
    for other in (across, sibling):
        pl.semaphore_signal(barrier, inc=1, device_id={"expert": other}, device_id_type=MESH)
    for other in along_z + along_x + along_y:
        pl.semaphore_signal(barrier, inc=1, device_id={"node": other}, device_id_type=MESH)

    for load in loads:
        load.start()

    def down_load(b):
        cols = pl.ds(pl.multiple_of(b * LANES, LANES), LANES)
        dst = down_wide.at[pl.ds(pl.multiple_of(b * hid, hid), hid)]
        return pltpu.make_async_copy(param_down.at[:, cols], dst, block_sem.at[b])

    @pl.loop(0, width // LANES)
    def _(b):
        down_load(b).start()

    pl.semaphore_wait(barrier, 2 + len(along_z + along_x + along_y))

    def token_copy(p, way, src, dst, other):
        return pltpu.make_async_remote_copy(
            src_ref=src,
            dst_ref=dst,
            send_sem=tok_send.at[way, p],
            recv_sem=tok_recv.at[way, p],
            device_id={"expert": other},
            device_id_type=MESH,
        )

    to_sibling = [token_copy(p, 0, slot(p, 0), slot(p, 1), sibling) for p in range(len(pieces))]
    to_across = [token_copy(p, 1, slot(p, 0), slot(p, 2), across) for p in range(len(pieces))]
    onward = [token_copy(p, 2, slot(p, 2), slot(p, 3), sibling) for p in range(len(pieces))]
    for p in range(len(pieces)):
        loads[p].wait()
        to_across[p].start()
        to_sibling[p].start()

    rounds = [along_z] * (zs // 2) + [along_x] * (X_SIZE // 2) + [along_y]
    for r, others in enumerate(rounds):
        for other in others:
            pl.semaphore_signal(
                enter_sem.at[r], inc=1, device_id={"node": other}, device_id_type=MESH
            )
        pl.semaphore_wait(enter_sem.at[r], len(others))

    loads[-1].wait()

    @pl.loop(0, width // TILE)
    def _(k):
        span = pl.ds(pl.multiple_of(k * TILE, TILE), TILE)
        gu_short[span, :] = gu_wide[span, :].astype(jnp.bfloat16)

    @pl.loop(0, width // LANES)
    def _(b):
        down_load(b).wait()
        cols = pl.ds(pl.multiple_of(b * LANES, LANES), LANES)
        block = down_wide[pl.ds(pl.multiple_of(b * hid, hid), hid), :]
        down_short[:, cols] = block.astype(jnp.bfloat16)

    both[...] = jnp.zeros_like(both)
    dact[...] = jnp.zeros_like(dact)

    def arrive(p):
        to_across[p].wait_recv()
        onward[p].start()
        to_sibling[p].wait_recv()
        onward[p].wait_recv()

    def turn(p):
        @pl.loop(p * (x_cols // 256), (p + 1) * (x_cols // 256))
        def _(k):
            span = pl.ds(pl.multiple_of(k * 256, 256), 256)
            x_turned[span, :] = x_all[:, span].T

    arrive(0)
    for p in range(X_PARTS):
        arrive(1 + p)

        @pl.loop(p * (x_cols // TILE), (p + 1) * (x_cols // TILE))
        def _(k):
            span = pl.ds(pl.multiple_of(k * TILE, TILE), TILE)
            both[...] += jnp.dot(
                x_all[:, span], gu_short[span, :], preferred_element_type=jnp.float32
            )

        if p < X_PARTS - 1:
            turn(p)

    def picked_at(s):
        named = codes[s]
        hit = jnp.where((named[0:1, :] == expert) | (named[1:2, :] == expert), 1, 0)
        return jnp.broadcast_to(hit, (rows, rows)).T != 0

    in_scale = 1.0 / math.sqrt(width)
    hid_scale = 1.0 / math.sqrt(hid)
    first = lax.broadcasted_iota(jnp.int32, (hid, hid), 0)
    second = lax.broadcasted_iota(jnp.int32, (hid, hid), 1)
    wanted = jnp.where(first < hid // 2, 2 * first, 2 * first - (hid - 1))
    order = jnp.where(second == wanted, 1.0, 0.0).astype(jnp.bfloat16)
    for s in range(experts):
        part = pl.ds(s * rows, rows)
        gate = both[part, :hid] * in_scale
        upper = both[part, hid:] * in_scale
        act = jnp.where(picked_at(s), gate * jax.nn.sigmoid(gate) * upper, 0.0)
        act_turned[:, part] = lax.dot_general(
            order,
            act.astype(jnp.bfloat16),
            (((1,), (1,)), ((), ())),
            preferred_element_type=jnp.float32,
        ).astype(jnp.bfloat16)

    def exchange(t, src, dst, sems, c):
        return pltpu.make_async_remote_copy(
            src_ref=src,
            dst_ref=dst,
            send_sem=sems.at[0, c],
            recv_sem=sems.at[1, c],
            device_id={"node": t},
            device_id_type=MESH,
        )

    def gu_out(peer, c):
        return exchange(
            peer, send_gu.at[peer, pl.ds(c * gu_part, gu_part)], got_gu[c].at[me], gu_sem, c
        )

    spot = z * X_SIZE + x
    over = along_y[0]

    def some(ref, first, count, sems, c):
        most = ref.at[pl.ds(first, count)]
        return exchange((me + 1) % nodes, most, most, sems, c)

    def whole(got, sems, c):
        return some(got, 0, nodes - 1, sems, c)

    def down_out(peer, c):
        return exchange(peer, send_down[c].at[peer], got_down[c].at[me], down_sem, c)

    def down_relay(peer, c):
        other = peer - y * X_SIZE + (1 - y) * X_SIZE
        return exchange(peer, send_down[c].at[other], relay_down[c].at[spot], relay_sem, c)

    def down_over(k, c):
        return exchange(
            over,
            relay_down[c].at[pl.ds(k * X_SIZE, X_SIZE)],
            got_down[c].at[pl.ds(k * plane + y * X_SIZE, X_SIZE)],
            over_sem,
            c,
        )

    def send_row(c):
        def both_ways(peer):
            down_out(peer, c).start()
            down_relay(peer, c).start()

        @pl.loop(1, X_SIZE)
        def _(k):
            both_ways(z_bases[0] + y * X_SIZE + (x + k) % X_SIZE)

        @pl.loop(0, X_SIZE)
        def _(k):
            here = y * X_SIZE + (x + k) % X_SIZE
            for base in z_bases[1:]:
                both_ways(base + here)

    for c in range(DY_PARTS):
        arrive(1 + X_PARTS + c)
        blocks = DY_BLOCKS[c]
        down_part = 2 * blocks

        @pl.loop(0, blocks * LANES // TILE)
        def _(k):
            at = pl.multiple_of(starts[c] * LANES + k * TILE, TILE)
            span = pl.ds(at, TILE)
            dact[...] += lax.dot_general(
                dy_all[:, span],
                down_short[:, span],
                (((1,), (1,)), ((), ())),
                preferred_element_type=jnp.float32,
            )
            grad = jnp.dot(act_turned[...], dy_all[:, span], preferred_element_type=jnp.float32)
            grad = grad * (0.5 * hid_scale)
            for r in range(2):
                for i in range(TILE // LANES):
                    block = starts[c] + k * (TILE // LANES) + i
                    old = down_wide[pl.ds(block * hid + r, nodes, stride=2), :]
                    new = old - grad[r * nodes : (r + 1) * nodes, i * LANES : (i + 1) * LANES]
                    row = r * blocks + k * (TILE // LANES) + i
                    stage[pl.ds(row, nodes, stride=down_part), :] = new

        @pl.loop(0, nodes)
        def _(n):
            span = pl.ds(pl.multiple_of(n * down_part, down_part), down_part)
            send_down[c][n] = stage[span, :].astype(jnp.bfloat16)

        send_row(c)
        got_down[c][me] = send_down[c][me]
        relay_down[c][spot] = send_down[c][over]
        if c == 1:
            turn(X_PARTS - 1)

    for s in range(experts):
        part = pl.ds(s * rows, rows)
        gate = both[part, :hid] * in_scale
        upper = both[part, hid:] * in_scale
        sigma = jax.nn.sigmoid(gate)
        da = dact[part, :] * hid_scale
        picked = picked_at(s)
        dgate = da * upper * sigma * (1.0 + gate * (1.0 - sigma))
        dupper = da * gate * sigma
        dboth[part, :hid] = jnp.where(picked, dgate, 0.0).astype(jnp.bfloat16)
        dboth[part, hid:] = jnp.where(picked, dupper, 0.0).astype(jnp.bfloat16)

    @pl.loop(0, zs)
    def _(j):
        zt = (z + (j % 2) * ((j + 1) // 2) + (1 - j % 2) * (zs - j // 2)) % zs
        at = pl.multiple_of(zt * (plane * gu_rows), plane * gu_rows)
        span = pl.ds(at, plane * gu_rows)
        grad = jnp.dot(x_turned[span, :], dboth[...], preferred_element_type=jnp.float32)
        new = gu_wide[span, :] - grad * (0.5 * in_scale)
        send_gu[pl.ds(zt * plane, plane)] = new.astype(jnp.bfloat16).reshape(
            plane, gu_rows, new.shape[1]
        )
        for k in range(plane):
            peer = zt * plane + in_plane(k)
            if k == 0:

                @pl.when(j > 0)
                def _():
                    gu_out(peer, 0).start()

            else:
                gu_out(peer, 0).start()

    for c in range(DY_PARTS):
        some(relay_down[c], 1, nodes // Y_LO - 1, relay_sem, c).wait_recv()

        @pl.loop(0, zs)
        def _(k):
            down_over(k, c).start()

    for c in range(1, GU_PARTS):

        each_peer(lambda peer: gu_out(peer, c).start())

    for c in range(GU_PARTS):
        got_gu[c][me] = send_gu[me, pl.ds(c * gu_part, gu_part)]

    def shift_at(i):
        exponent, shift = plan[i], jnp.int32(1)
        for e in range(1, SHIFTS):
            shift = jnp.where(exponent == e, jnp.int32(1 << e), shift)
        return shift

    s0, s1, s2, s3 = (shift_at(i) for i in range(ROUNDS))

    def filtered(got, half, done, mean):
        def wide(index):
            return got[lax.rem(index, nodes)].astype(jnp.float32)

        def early(n, total):
            own = wide(n)
            half[n] = (own + wide(n + s0)) + (wide(n + s1) + wide(n + s0 + s1))
            return total + own

        total = lax.fori_loop(0, nodes, early, jnp.zeros(half.shape[1:], jnp.float32), unroll=2)
        mean[...] = total * (1.0 / nodes)

        def late(n, carry):
            value = (half[n] + half[lax.rem(n + s2, nodes)]) + (
                half[lax.rem(n + s3, nodes)] + half[lax.rem(n + s2 + s3, nodes)]
            )
            done[n] = (value * (1.0 / 16.0)).astype(jnp.bfloat16)
            return carry

        lax.fori_loop(0, nodes, late, 0, unroll=2)

    def gu_home(peer, c):
        dst = out_gu.at[me, pl.ds(c * gu_part, gu_part)]
        return exchange(peer, done_gu.at[c, peer], dst, gu_sem, GU_PARTS + c)

    def down_home(peer, c):
        return exchange(
            peer, done_down[c].at[peer], home_down[c].at[me], down_sem, DY_PARTS + c
        )

    def put_down(c):
        cols = pl.ds(starts[c] * LANES, DY_BLOCKS[c] * LANES)
        return pltpu.make_async_copy(last_down[c], out_down.at[:, cols], keep_down.at[c])

    def own_gu(c):
        dst = out_gu.at[me, pl.ds(c * gu_part, gu_part)]
        return pltpu.make_async_copy(done_gu.at[c, me], dst, keep_gu.at[c])

    for c in range(DY_PARTS):
        some(got_down[c], 0, nodes // Y_LO - 1, down_sem, c).wait_recv()
        some(got_down[c], 0, nodes // Y_LO, over_sem, c).wait_recv()
        blocks = DY_BLOCKS[c]
        filtered(
            got_down[c],
            half_down.at[:, pl.ds(0, 2 * blocks)],
            done_down[c],
            mean_stage.at[pl.ds(0, 2 * blocks)],
        )
        for r in range(2):
            for i in range(blocks):
                at = (starts[c] + i) * LANES
                mean_rows[r : r + 1, at : at + LANES] = mean_stage[
                    r * blocks + i : r * blocks + i + 1, :
                ]

        each_peer(lambda peer: down_home(peer, c).start())

        home_down[c][me] = done_down[c][me]

    for c in range(GU_PARTS):
        whole(got_gu[c], gu_sem, c).wait_recv()
        filtered(
            got_gu[c], half_gu, done_gu.at[c], mean_slab.at[pl.ds(c * gu_part, gu_part)]
        )

        each_peer(lambda peer: gu_home(peer, c).start())

        own_gu(c).start()

    means = [
        pltpu.make_async_copy(mean_slab, mean_gu, mean_sem.at[0]),
        pltpu.make_async_copy(mean_rows, mean_down, mean_sem.at[1]),
    ]
    for copy in means:
        copy.start()

    for c in range(DY_PARTS):
        whole(got_down[c], down_sem, DY_PARTS + c).wait_recv()
        blocks = DY_BLOCKS[c]
        down_part = 2 * blocks

        @pl.loop(0, nodes)
        def _(n):
            span = pl.ds(pl.multiple_of(n * down_part, down_part), down_part)
            stage[span, :] = home_down[c][n].astype(jnp.float32)

        for i in range(blocks):
            for r in range(2):
                row = r * blocks + i
                turned[pl.ds(i * hid + r, nodes, stride=2), :] = stage[
                    pl.ds(row, nodes, stride=down_part), :
                ]
            last_down[c][:, i * LANES : (i + 1) * LANES] = turned[
                i * hid : (i + 1) * hid, :
            ].astype(jnp.bfloat16)
        put_down(c).start()

    for copy in means:
        copy.wait()
    for p in range(len(pieces)):
        to_sibling[p].wait_send()
        to_across[p].wait_send()
        onward[p].wait_send()
    for c in range(DY_PARTS):
        some(got_down[c], 0, nodes // Y_LO - 1, down_sem, c).wait_send()
        some(relay_down[c], 1, nodes // Y_LO - 1, relay_sem, c).wait_send()
        some(got_down[c], 0, nodes // Y_LO, over_sem, c).wait_send()
        whole(got_down[c], down_sem, DY_PARTS + c).wait_send()
        put_down(c).wait()
    for c in range(GU_PARTS):
        whole(got_gu[c], gu_sem, c).wait_send()
        whole(got_gu[c], gu_sem, GU_PARTS + c).wait_send()
        whole(got_gu[c], gu_sem, GU_PARTS + c).wait_recv()
        own_gu(c).wait()


def put_out(*refs):
    sems = refs[-1]
    copies = [pltpu.make_async_copy(refs[i], refs[4 + i], sems.at[i]) for i in range(4)]
    for copy in copies:
        copy.start()
    for copy in copies:
        copy.wait()


def step(param_gu, param_down, tokens, cotangent, routes, plan):
    nodes = lax.axis_size("node")
    experts = lax.axis_size("expert")
    rows, width = tokens.shape
    cols = param_gu.shape[1]
    hid = param_down.shape[0]
    gu_rows = width // nodes
    down_part = 2 * max(DY_BLOCKS)
    pieces = X_PARTS + 1 + DY_PARTS
    everywhere = pl.BlockSpec(memory_space=pl.ANY)
    outside = pl.BlockSpec(memory_space=pltpu.HBM)
    short, wide = jnp.bfloat16, jnp.float32

    def body(*refs):
        kernel_body(nodes, *refs)

    held = [
        pltpu.with_memory_space_constraint(a, pltpu.HBM)
        for a in (routes.T, tokens, cotangent, param_gu, param_down)
    ]
    mixed_gu, mixed_down, mean_gu, mean_down = pl.pallas_call(
        body,
        out_shape=(
            jax.ShapeDtypeStruct((nodes, gu_rows, cols), short),
            jax.ShapeDtypeStruct((hid, width), short),
            jax.ShapeDtypeStruct((gu_rows, cols), wide),
            jax.ShapeDtypeStruct((hid // nodes, width), wide),
        ),
        in_specs=[pl.BlockSpec(memory_space=pltpu.SMEM)] + [outside] * 5,
        out_specs=(everywhere,) * 4,
        scratch_shapes=[
            pltpu.VMEM((experts * rows, width), short),
            pltpu.VMEM((experts * rows, width), short),
            pltpu.VMEM((width, experts * rows), short),
            pltpu.VMEM((width, cols), wide),
            pltpu.VMEM((hid * width // LANES, LANES), wide),
            pltpu.VMEM((width, cols), short),
            pltpu.VMEM((hid, width), short),
            pltpu.VMEM((experts * rows, cols), wide),
            pltpu.VMEM((experts * rows, hid), wide),
            pltpu.VMEM((hid, experts * rows), short),
            pltpu.VMEM((experts * rows, cols), short),
            pltpu.VMEM((experts, 2, rows), jnp.int32),
            pltpu.VMEM((nodes * down_part, LANES), wide),
            pltpu.VMEM((nodes * down_part, LANES), wide),
            pltpu.VMEM((down_part, LANES), wide),
            pltpu.VMEM((hid // nodes, width), wide),
            pltpu.VMEM((gu_rows, cols), wide),
            pltpu.SemaphoreType.DMA((2,)),
            pltpu.VMEM((nodes, gu_rows // GU_PARTS, cols), wide),
            pltpu.VMEM((nodes, down_part, LANES), wide),
            pltpu.VMEM((nodes, gu_rows, cols), short),
            pltpu.VMEM((GU_PARTS, nodes, gu_rows // GU_PARTS, cols), short),
            pltpu.SemaphoreType.REGULAR((nodes // (Y_LO * X_SIZE) // 2 + X_SIZE // 2 + 1,)),
            pltpu.SemaphoreType.DMA((1 + pieces,)),
            pltpu.SemaphoreType.DMA((width // LANES,)),
            pltpu.SemaphoreType.DMA((3, pieces)),
            pltpu.SemaphoreType.DMA((3, pieces)),
            pltpu.SemaphoreType.DMA((2, 2 * GU_PARTS)),
            pltpu.SemaphoreType.DMA((2, 2 * DY_PARTS)),
            pltpu.SemaphoreType.DMA((2, DY_PARTS)),
            pltpu.SemaphoreType.DMA((2, DY_PARTS)),
            pltpu.SemaphoreType.DMA((GU_PARTS,)),
            pltpu.SemaphoreType.DMA((DY_PARTS,)),
        ]
        + [pltpu.VMEM((nodes, gu_rows // GU_PARTS, cols), short)] * GU_PARTS
        + [pltpu.VMEM((nodes, 2 * b, LANES), short) for b in DY_BLOCKS] * 4
        + [pltpu.VMEM((nodes // Y_LO, 2 * b, LANES), short) for b in DY_BLOCKS]
        + [pltpu.VMEM((hid, b * LANES), short) for b in DY_BLOCKS],
        compiler_params=pltpu.CompilerParams(
            collective_id=1, has_side_effects=True, vmem_limit_bytes=48 * 1024 * 1024
        ),
        name="expert_gossip",
    )(plan, *held)

    results = (mixed_gu.reshape(width, cols), mixed_down, mean_gu, mean_down)
    return pl.pallas_call(
        put_out,
        out_shape=tuple(jax.ShapeDtypeStruct(a.shape, a.dtype) for a in results),
        in_specs=[pl.BlockSpec(memory_space=pltpu.VMEM)] * 4,
        out_specs=(outside,) * 4,
        scratch_shapes=[pltpu.SemaphoreType.DMA((4,))],
        compiler_params=pltpu.CompilerParams(vmem_limit_bytes=1024 * 1024),
        name="put_out",
    )(*results)


def solution(mesh):
    both = P(("node", "expert"), None)
    split = P("node", "expert")
    return jax.shard_map(
        step,
        mesh=mesh,
        in_specs=(split, split, both, both, both, P()),
        out_specs=(split, split, split, split),
        check_vma=False,
    )
```

```python
import math

import jax
import jax.numpy as jnp
from jax import lax
from jax.experimental import pallas as pl
from jax.experimental.pallas import tpu as pltpu
from jax.sharding import PartitionSpec as P

MESH = pl.DeviceIdType.MESH
ROUNDS = 4
SHIFTS = 6
X_BLOCKS = (8, 8, 8, 4, 4)
X_PARTS = len(X_BLOCKS)
DY_BLOCKS = (4,) * 8
DY_PARTS = len(DY_BLOCKS)
GU_PARTS = 4
LANES = 128
TILE = 512
Y_LO, X_SIZE = 2, 4


def kernel_body(
    nodes,
    plan_in,
    routes,
    tokens,
    cotangent,
    param_gu,
    param_down,
    out_gu,
    out_down,
    mean_gu,
    mean_down,
    x_all,
    dy_all,
    x_turned,
    gu_wide,
    down_wide,
    gu_short,
    down_short,
    both,
    dact,
    act_turned,
    dboth,
    codes,
    stage,
    turned,
    mean_stage,
    mean_rows,
    mean_slab,
    mean_sem,
    plan,
    plan_sem,
    half_gu,
    half_down,
    send_gu,
    done_gu,
    enter_sem,
    local_sem,
    block_sem,
    tok_send,
    tok_recv,
    gu_sem,
    down_sem,
    relay_sem,
    over_sem,
    keep_gu,
    keep_down,
    *landing,
):
    got_gu, downs = landing[:GU_PARTS], landing[GU_PARTS:]
    send_down, got_down, done_down, home_down, relay_down, last_down = (
        downs[i * DY_PARTS : (i + 1) * DY_PARTS] for i in range(6)
    )
    me = lax.axis_index("node")
    expert = lax.axis_index("expert")
    experts = lax.axis_size("expert")
    plane = Y_LO * X_SIZE
    zs = nodes // plane
    z, y, x = me // plane, (me // X_SIZE) % Y_LO, me % X_SIZE
    sibling = expert + 1 - 2 * (expert % 2)
    across = (expert + 2) % experts
    rows, width = tokens.shape
    hid = param_down.shape[0]
    gu_rows = send_gu.shape[1]
    gu_part = gu_rows // GU_PARTS
    starts = [sum(DY_BLOCKS[:c]) for c in range(DY_PARTS)]

    steps = [0] + [d for j in range(1, zs // 2) for d in (j, zs - j)] + [zs // 2]
    z_bases = [((z + d) % zs) * plane for d in steps]

    def in_plane(k):
        return ((y + k // X_SIZE) % Y_LO) * X_SIZE + (x + k % X_SIZE) % X_SIZE

    def each_peer(send):
        @pl.loop(1, plane)
        def _(k):
            send(z_bases[0] + in_plane(k))

        @pl.loop(0, plane)
        def _(k):
            here = in_plane(k)
            for base in z_bases[1:]:
                send(base + here)

    x_starts = [sum(X_BLOCKS[:c]) for c in range(X_PARTS)]
    pieces = (
        [(routes, codes, None)]
        + [
            (tokens, x_all, pl.ds(x_starts[c] * LANES, X_BLOCKS[c] * LANES))
            for c in range(X_PARTS)
        ]
        + [
            (cotangent, dy_all, pl.ds(starts[c] * LANES, DY_BLOCKS[c] * LANES))
            for c in range(DY_PARTS)
        ]
    )

    def source(p):
        src, _, cols = pieces[p]
        return src if cols is None else src.at[:, cols]

    def slot(p, s):
        _, dst, cols = pieces[p]
        if cols is None:
            return dst.at[s]
        return dst.at[pl.ds(s * rows, rows), cols]

    loads = [
        pltpu.make_async_copy(source(p), slot(p, 0), local_sem.at[p]) for p in range(len(pieces))
    ]
    plan_load = pltpu.make_async_copy(plan_in, plan, plan_sem)
    loads.append(pltpu.make_async_copy(param_gu, gu_wide, local_sem.at[len(pieces)]))
    home = me % plane
    along_z = [((z + d) % zs) * plane + home for d in (1, zs - 1)]
    along_x = [me - x + (x + d) % X_SIZE for d in (1, X_SIZE - 1)]
    along_y = [me - y * X_SIZE + (1 - y) * X_SIZE]
    barrier = pltpu.get_barrier_semaphore()
    for other in (across, sibling):
        pl.semaphore_signal(barrier, inc=1, device_id={"expert": other}, device_id_type=MESH)
    for other in along_z + along_x + along_y:
        pl.semaphore_signal(barrier, inc=1, device_id={"node": other}, device_id_type=MESH)

    for load in loads:
        load.start()
    plan_load.start()

    def down_load(b):
        cols = pl.ds(pl.multiple_of(b * LANES, LANES), LANES)
        dst = down_wide.at[pl.ds(pl.multiple_of(b * hid, hid), hid)]
        return pltpu.make_async_copy(param_down.at[:, cols], dst, block_sem.at[b])

    @pl.loop(0, width // LANES)
    def _(b):
        down_load(b).start()

    pl.semaphore_wait(barrier, 2 + len(along_z + along_x + along_y))

    def token_copy(p, way, src, dst, other):
        return pltpu.make_async_remote_copy(
            src_ref=src,
            dst_ref=dst,
            send_sem=tok_send.at[way, p],
            recv_sem=tok_recv.at[way, p],
            device_id={"expert": other},
            device_id_type=MESH,
        )

    to_sibling = [token_copy(p, 0, slot(p, 0), slot(p, 1), sibling) for p in range(len(pieces))]
    to_across = [token_copy(p, 1, slot(p, 0), slot(p, 2), across) for p in range(len(pieces))]
    onward = [token_copy(p, 2, slot(p, 2), slot(p, 3), sibling) for p in range(len(pieces))]
    for p in range(len(pieces)):
        loads[p].wait()
        to_across[p].start()
        to_sibling[p].start()

    rounds = [along_z] * (zs // 2) + [along_x] * (X_SIZE // 2) + [along_y]
    for r, others in enumerate(rounds):
        for other in others:
            pl.semaphore_signal(
                enter_sem.at[r], inc=1, device_id={"node": other}, device_id_type=MESH
            )
        pl.semaphore_wait(enter_sem.at[r], len(others))

    loads[-1].wait()
    plan_load.wait()

    @pl.loop(0, width // TILE)
    def _(k):
        span = pl.ds(pl.multiple_of(k * TILE, TILE), TILE)
        gu_short[span, :] = gu_wide[span, :].astype(jnp.bfloat16)

    @pl.loop(0, width // LANES)
    def _(b):
        down_load(b).wait()
        cols = pl.ds(pl.multiple_of(b * LANES, LANES), LANES)
        block = down_wide[pl.ds(pl.multiple_of(b * hid, hid), hid), :]
        down_short[:, cols] = block.astype(jnp.bfloat16)

    both[...] = jnp.zeros_like(both)
    dact[...] = jnp.zeros_like(dact)

    def arrive(p):
        to_across[p].wait_recv()
        onward[p].start()
        to_sibling[p].wait_recv()
        onward[p].wait_recv()

    def turn(p):
        @pl.loop(x_starts[p] // 2, (x_starts[p] + X_BLOCKS[p]) // 2)
        def _(k):
            span = pl.ds(pl.multiple_of(k * 256, 256), 256)
            x_turned[span, :] = x_all[:, span].T

    arrive(0)
    for p in range(X_PARTS):
        arrive(1 + p)

        @pl.loop(x_starts[p] * LANES // TILE, (x_starts[p] + X_BLOCKS[p]) * LANES // TILE)
        def _(k):
            span = pl.ds(pl.multiple_of(k * TILE, TILE), TILE)
            both[...] += jnp.dot(
                x_all[:, span], gu_short[span, :], preferred_element_type=jnp.float32
            )

        if p < X_PARTS - 1:
            turn(p)

    def picked_at(s):
        named = codes[s]
        hit = jnp.where((named[0:1, :] == expert) | (named[1:2, :] == expert), 1, 0)
        return jnp.broadcast_to(hit, (rows, rows)).T != 0

    in_scale = 1.0 / math.sqrt(width)
    hid_scale = 1.0 / math.sqrt(hid)
    first = lax.broadcasted_iota(jnp.int32, (hid, hid), 0)
    second = lax.broadcasted_iota(jnp.int32, (hid, hid), 1)
    wanted = jnp.where(first < hid // 2, 2 * first, 2 * first - (hid - 1))
    order = jnp.where(second == wanted, 1.0, 0.0).astype(jnp.bfloat16)
    for s in range(experts):
        part = pl.ds(s * rows, rows)
        gate = both[part, :hid] * in_scale
        upper = both[part, hid:] * in_scale
        act = jnp.where(picked_at(s), gate * jax.nn.sigmoid(gate) * upper, 0.0)
        act_turned[:, part] = lax.dot_general(
            order,
            act.astype(jnp.bfloat16),
            (((1,), (1,)), ((), ())),
            preferred_element_type=jnp.float32,
        ).astype(jnp.bfloat16)

    def exchange(t, src, dst, sems, c):
        return pltpu.make_async_remote_copy(
            src_ref=src,
            dst_ref=dst,
            send_sem=sems.at[0, c],
            recv_sem=sems.at[1, c],
            device_id={"node": t},
            device_id_type=MESH,
        )

    def gu_out(peer, c):
        return exchange(
            peer, send_gu.at[peer, pl.ds(c * gu_part, gu_part)], got_gu[c].at[me], gu_sem, c
        )

    spot = z * X_SIZE + x
    over = along_y[0]

    def some(ref, first, count, sems, c):
        most = ref.at[pl.ds(first, count)]
        return exchange((me + 1) % nodes, most, most, sems, c)

    def whole(got, sems, c):
        return some(got, 0, nodes - 1, sems, c)

    def down_out(peer, c):
        return exchange(peer, send_down[c].at[peer], got_down[c].at[me], down_sem, c)

    def down_relay(peer, c):
        other = peer - y * X_SIZE + (1 - y) * X_SIZE
        return exchange(peer, send_down[c].at[other], relay_down[c].at[spot], relay_sem, c)

    def down_over(k, c):
        return exchange(
            over,
            relay_down[c].at[pl.ds(k * X_SIZE, X_SIZE)],
            got_down[c].at[pl.ds(k * plane + y * X_SIZE, X_SIZE)],
            over_sem,
            c,
        )

    def send_row(c):
        def both_ways(peer):
            down_out(peer, c).start()
            down_relay(peer, c).start()

        @pl.loop(1, X_SIZE)
        def _(k):
            both_ways(z_bases[0] + y * X_SIZE + (x + k) % X_SIZE)

        @pl.loop(0, X_SIZE)
        def _(k):
            here = y * X_SIZE + (x + k) % X_SIZE
            for base in z_bases[1:]:
                both_ways(base + here)

    for c in range(DY_PARTS):
        arrive(1 + X_PARTS + c)
        blocks = DY_BLOCKS[c]
        down_part = 2 * blocks

        @pl.loop(0, blocks * LANES // TILE)
        def _(k):
            at = pl.multiple_of(starts[c] * LANES + k * TILE, TILE)
            span = pl.ds(at, TILE)
            dact[...] += lax.dot_general(
                dy_all[:, span],
                down_short[:, span],
                (((1,), (1,)), ((), ())),
                preferred_element_type=jnp.float32,
            )
            grad = jnp.dot(act_turned[...], dy_all[:, span], preferred_element_type=jnp.float32)
            grad = grad * (0.5 * hid_scale)
            for r in range(2):
                for i in range(TILE // LANES):
                    block = starts[c] + k * (TILE // LANES) + i
                    old = down_wide[pl.ds(block * hid + r, nodes, stride=2), :]
                    new = old - grad[r * nodes : (r + 1) * nodes, i * LANES : (i + 1) * LANES]
                    row = r * blocks + k * (TILE // LANES) + i
                    stage[pl.ds(row, nodes, stride=down_part), :] = new

        @pl.loop(0, nodes)
        def _(n):
            span = pl.ds(pl.multiple_of(n * down_part, down_part), down_part)
            send_down[c][n] = stage[span, :].astype(jnp.bfloat16)

        send_row(c)
        got_down[c][me] = send_down[c][me]
        relay_down[c][spot] = send_down[c][over]
        if c == 1:
            turn(X_PARTS - 1)

    for s in range(experts):
        part = pl.ds(s * rows, rows)
        gate = both[part, :hid] * in_scale
        upper = both[part, hid:] * in_scale
        sigma = jax.nn.sigmoid(gate)
        da = dact[part, :] * hid_scale
        picked = picked_at(s)
        dgate = da * upper * sigma * (1.0 + gate * (1.0 - sigma))
        dupper = da * gate * sigma
        dboth[part, :hid] = jnp.where(picked, dgate, 0.0).astype(jnp.bfloat16)
        dboth[part, hid:] = jnp.where(picked, dupper, 0.0).astype(jnp.bfloat16)

    @pl.loop(0, zs)
    def _(j):
        zt = (z + (j % 2) * ((j + 1) // 2) + (1 - j % 2) * (zs - j // 2)) % zs
        at = pl.multiple_of(zt * (plane * gu_rows), plane * gu_rows)
        span = pl.ds(at, plane * gu_rows)
        grad = jnp.dot(x_turned[span, :], dboth[...], preferred_element_type=jnp.float32)
        new = gu_wide[span, :] - grad * (0.5 * in_scale)
        send_gu[pl.ds(zt * plane, plane)] = new.astype(jnp.bfloat16).reshape(
            plane, gu_rows, new.shape[1]
        )
        for k in range(plane):
            peer = zt * plane + in_plane(k)
            if k == 0:

                @pl.when(j > 0)
                def _():
                    gu_out(peer, 0).start()

            else:
                gu_out(peer, 0).start()

    for c in range(DY_PARTS):
        some(relay_down[c], 1, nodes // Y_LO - 1, relay_sem, c).wait_recv()

        @pl.loop(0, zs)
        def _(k):
            down_over(k, c).start()

    for c in range(1, GU_PARTS):

        each_peer(lambda peer: gu_out(peer, c).start())

    for c in range(GU_PARTS):
        got_gu[c][me] = send_gu[me, pl.ds(c * gu_part, gu_part)]

    def shift_at(i):
        exponent, shift = plan[i], jnp.int32(1)
        for e in range(1, SHIFTS):
            shift = jnp.where(exponent == e, jnp.int32(1 << e), shift)
        return shift

    s0, s1, s2, s3 = (shift_at(i) for i in range(ROUNDS))

    def filtered(got, half, done, mean):
        def wide(index):
            return got[lax.rem(index, nodes)].astype(jnp.float32)

        def early(n, total):
            own = wide(n)
            half[n] = (own + wide(n + s0)) + (wide(n + s1) + wide(n + s0 + s1))
            return total + own

        total = lax.fori_loop(0, nodes, early, jnp.zeros(half.shape[1:], jnp.float32), unroll=2)
        mean[...] = total * (1.0 / nodes)

        def late(n, carry):
            value = (half[n] + half[lax.rem(n + s2, nodes)]) + (
                half[lax.rem(n + s3, nodes)] + half[lax.rem(n + s2 + s3, nodes)]
            )
            done[n] = (value * (1.0 / 16.0)).astype(jnp.bfloat16)
            return carry

        lax.fori_loop(0, nodes, late, 0, unroll=2)

    def gu_home(peer, c):
        dst = out_gu.at[me, pl.ds(c * gu_part, gu_part)]
        return exchange(peer, done_gu.at[c, peer], dst, gu_sem, GU_PARTS + c)

    def down_home(peer, c):
        return exchange(
            peer, done_down[c].at[peer], home_down[c].at[me], down_sem, DY_PARTS + c
        )

    def put_down(c):
        cols = pl.ds(starts[c] * LANES, DY_BLOCKS[c] * LANES)
        return pltpu.make_async_copy(last_down[c], out_down.at[:, cols], keep_down.at[c])

    def own_gu(c):
        dst = out_gu.at[me, pl.ds(c * gu_part, gu_part)]
        return pltpu.make_async_copy(done_gu.at[c, me], dst, keep_gu.at[c])

    for c in range(DY_PARTS):
        some(got_down[c], 0, nodes // Y_LO - 1, down_sem, c).wait_recv()
        some(got_down[c], 0, nodes // Y_LO, over_sem, c).wait_recv()
        blocks = DY_BLOCKS[c]
        filtered(
            got_down[c],
            half_down.at[:, pl.ds(0, 2 * blocks)],
            done_down[c],
            mean_stage.at[pl.ds(0, 2 * blocks)],
        )
        for r in range(2):
            for i in range(blocks):
                at = (starts[c] + i) * LANES
                mean_rows[r : r + 1, at : at + LANES] = mean_stage[
                    r * blocks + i : r * blocks + i + 1, :
                ]

        each_peer(lambda peer: down_home(peer, c).start())

        home_down[c][me] = done_down[c][me]

    for c in range(GU_PARTS):
        whole(got_gu[c], gu_sem, c).wait_recv()
        filtered(
            got_gu[c], half_gu, done_gu.at[c], mean_slab.at[pl.ds(c * gu_part, gu_part)]
        )

        each_peer(lambda peer: gu_home(peer, c).start())

        own_gu(c).start()

    means = [
        pltpu.make_async_copy(mean_slab, mean_gu, mean_sem.at[0]),
        pltpu.make_async_copy(mean_rows, mean_down, mean_sem.at[1]),
    ]
    for copy in means:
        copy.start()

    for c in range(DY_PARTS):
        whole(got_down[c], down_sem, DY_PARTS + c).wait_recv()
        blocks = DY_BLOCKS[c]
        down_part = 2 * blocks

        @pl.loop(0, nodes)
        def _(n):
            span = pl.ds(pl.multiple_of(n * down_part, down_part), down_part)
            stage[span, :] = home_down[c][n].astype(jnp.float32)

        for i in range(blocks):
            for r in range(2):
                row = r * blocks + i
                turned[pl.ds(i * hid + r, nodes, stride=2), :] = stage[
                    pl.ds(row, nodes, stride=down_part), :
                ]
            last_down[c][:, i * LANES : (i + 1) * LANES] = turned[
                i * hid : (i + 1) * hid, :
            ].astype(jnp.bfloat16)
        put_down(c).start()

    for copy in means:
        copy.wait()
    for p in range(len(pieces)):
        to_sibling[p].wait_send()
        to_across[p].wait_send()
        onward[p].wait_send()
    for c in range(DY_PARTS):
        some(got_down[c], 0, nodes // Y_LO - 1, down_sem, c).wait_send()
        some(relay_down[c], 1, nodes // Y_LO - 1, relay_sem, c).wait_send()
        some(got_down[c], 0, nodes // Y_LO, over_sem, c).wait_send()
        whole(got_down[c], down_sem, DY_PARTS + c).wait_send()
        put_down(c).wait()
    for c in range(GU_PARTS):
        whole(got_gu[c], gu_sem, c).wait_send()
        whole(got_gu[c], gu_sem, GU_PARTS + c).wait_send()
        whole(got_gu[c], gu_sem, GU_PARTS + c).wait_recv()
        own_gu(c).wait()


def put_out(*refs):
    sems = refs[-1]
    copies = [pltpu.make_async_copy(refs[i], refs[4 + i], sems.at[i]) for i in range(4)]
    for copy in copies:
        copy.start()
    for copy in copies:
        copy.wait()


def step(param_gu, param_down, tokens, cotangent, routes, plan):
    nodes = lax.axis_size("node")
    experts = lax.axis_size("expert")
    rows, width = tokens.shape
    cols = param_gu.shape[1]
    hid = param_down.shape[0]
    gu_rows = width // nodes
    down_part = 2 * max(DY_BLOCKS)
    pieces = X_PARTS + 1 + DY_PARTS
    everywhere = pl.BlockSpec(memory_space=pl.ANY)
    outside = pl.BlockSpec(memory_space=pltpu.HBM)
    short, wide = jnp.bfloat16, jnp.float32

    def body(*refs):
        kernel_body(nodes, *refs)

    held = [
        pltpu.with_memory_space_constraint(a, pltpu.HBM)
        for a in (plan, routes.T, tokens, cotangent, param_gu, param_down)
    ]
    mixed_gu, mixed_down, mean_gu, mean_down = pl.pallas_call(
        body,
        out_shape=(
            jax.ShapeDtypeStruct((nodes, gu_rows, cols), short),
            jax.ShapeDtypeStruct((hid, width), short),
            jax.ShapeDtypeStruct((gu_rows, cols), wide),
            jax.ShapeDtypeStruct((hid // nodes, width), wide),
        ),
        in_specs=[outside] * 6,
        out_specs=(everywhere,) * 4,
        scratch_shapes=[
            pltpu.VMEM((experts * rows, width), short),
            pltpu.VMEM((experts * rows, width), short),
            pltpu.VMEM((width, experts * rows), short),
            pltpu.VMEM((width, cols), wide),
            pltpu.VMEM((hid * width // LANES, LANES), wide),
            pltpu.VMEM((width, cols), short),
            pltpu.VMEM((hid, width), short),
            pltpu.VMEM((experts * rows, cols), wide),
            pltpu.VMEM((experts * rows, hid), wide),
            pltpu.VMEM((hid, experts * rows), short),
            pltpu.VMEM((experts * rows, cols), short),
            pltpu.VMEM((experts, 2, rows), jnp.int32),
            pltpu.VMEM((nodes * down_part, LANES), wide),
            pltpu.VMEM((nodes * down_part, LANES), wide),
            pltpu.VMEM((down_part, LANES), wide),
            pltpu.VMEM((hid // nodes, width), wide),
            pltpu.VMEM((gu_rows, cols), wide),
            pltpu.SemaphoreType.DMA((2,)),
            pltpu.SMEM((ROUNDS,), jnp.int32),
            pltpu.SemaphoreType.DMA(()),
            pltpu.VMEM((nodes, gu_rows // GU_PARTS, cols), wide),
            pltpu.VMEM((nodes, down_part, LANES), wide),
            pltpu.VMEM((nodes, gu_rows, cols), short),
            pltpu.VMEM((GU_PARTS, nodes, gu_rows // GU_PARTS, cols), short),
            pltpu.SemaphoreType.REGULAR((nodes // (Y_LO * X_SIZE) // 2 + X_SIZE // 2 + 1,)),
            pltpu.SemaphoreType.DMA((1 + pieces,)),
            pltpu.SemaphoreType.DMA((width // LANES,)),
            pltpu.SemaphoreType.DMA((3, pieces)),
            pltpu.SemaphoreType.DMA((3, pieces)),
            pltpu.SemaphoreType.DMA((2, 2 * GU_PARTS)),
            pltpu.SemaphoreType.DMA((2, 2 * DY_PARTS)),
            pltpu.SemaphoreType.DMA((2, DY_PARTS)),
            pltpu.SemaphoreType.DMA((2, DY_PARTS)),
            pltpu.SemaphoreType.DMA((GU_PARTS,)),
            pltpu.SemaphoreType.DMA((DY_PARTS,)),
        ]
        + [pltpu.VMEM((nodes, gu_rows // GU_PARTS, cols), short)] * GU_PARTS
        + [pltpu.VMEM((nodes, 2 * b, LANES), short) for b in DY_BLOCKS] * 4
        + [pltpu.VMEM((nodes // Y_LO, 2 * b, LANES), short) for b in DY_BLOCKS]
        + [pltpu.VMEM((hid, b * LANES), short) for b in DY_BLOCKS],
        compiler_params=pltpu.CompilerParams(
            collective_id=1, has_side_effects=True, vmem_limit_bytes=48 * 1024 * 1024
        ),
        name="expert_gossip",
    )(*held)

    results = (mixed_gu.reshape(width, cols), mixed_down, mean_gu, mean_down)
    return pl.pallas_call(
        put_out,
        out_shape=tuple(jax.ShapeDtypeStruct(a.shape, a.dtype) for a in results),
        in_specs=[pl.BlockSpec(memory_space=pltpu.VMEM)] * 4,
        out_specs=(outside,) * 4,
        scratch_shapes=[pltpu.SemaphoreType.DMA((4,))],
        compiler_params=pltpu.CompilerParams(vmem_limit_bytes=1024 * 1024),
        name="put_out",
    )(*results)


def solution(mesh):
    both = P(("node", "expert"), None)
    split = P("node", "expert")
    return jax.shard_map(
        step,
        mesh=mesh,
        in_specs=(split, split, both, both, both, P()),
        out_specs=(split, split, split, split),
        check_vma=False,
    )
```

```python
import math

import jax
import jax.numpy as jnp
from jax import lax
from jax.experimental import pallas as pl
from jax.experimental.pallas import tpu as pltpu
from jax.sharding import PartitionSpec as P

MESH = pl.DeviceIdType.MESH
ROUNDS = 4
SHIFTS = 6
X_BLOCKS = (8, 8, 8, 4, 4)
X_PARTS = len(X_BLOCKS)
DY_BLOCKS = (4,) * 8
DY_PARTS = len(DY_BLOCKS)
GU_PARTS = 4
LANES = 128
TILE = 512
Y_LO, X_SIZE = 2, 4


def kernel_body(
    nodes,
    plan_in,
    routes,
    tokens,
    cotangent,
    param_gu,
    param_down,
    out_gu,
    out_down,
    mean_gu,
    mean_down,
    x_all,
    dy_all,
    x_turned,
    gu_wide,
    down_wide,
    gu_short,
    down_short,
    both,
    dact,
    act_turned,
    dboth,
    codes,
    stage,
    turned,
    mean_stage,
    plan,
    half_gu,
    half_down,
    send_gu,
    done_gu,
    enter_sem,
    local_sem,
    tok_send,
    beside_sem,
    across_sem,
    onward_sem,
    link_sem,
    gu_in,
    down_in,
    relay_in,
    home_sem,
    *landing,
):
    got_gu, downs = landing[:GU_PARTS], landing[GU_PARTS:]
    send_down, got_down, done_down, home_down, relay_down = (
        downs[i * DY_PARTS : (i + 1) * DY_PARTS] for i in range(5)
    )
    me = lax.axis_index("node")
    expert = lax.axis_index("expert")
    experts = lax.axis_size("expert")
    plane = Y_LO * X_SIZE
    zs = nodes // plane
    z, y, x = me // plane, (me // X_SIZE) % Y_LO, me % X_SIZE
    sibling = expert + 1 - 2 * (expert % 2)
    across = (expert + 2) % experts
    rows, width = tokens.shape
    hid = param_down.shape[0]
    gu_rows = send_gu.shape[1]
    gu_part = gu_rows // GU_PARTS
    starts = [sum(DY_BLOCKS[:c]) for c in range(DY_PARTS)]

    steps = [0] + [d for j in range(1, zs // 2) for d in (j, zs - j)] + [zs // 2]
    z_bases = [((z + d) % zs) * plane for d in steps]

    def in_plane(k):
        return ((y + k // X_SIZE) % Y_LO) * X_SIZE + (x + k % X_SIZE) % X_SIZE

    def each_peer(send):
        @pl.loop(1, plane)
        def _(k):
            send(z_bases[0] + in_plane(k))

        @pl.loop(0, plane)
        def _(k):
            here = in_plane(k)
            for base in z_bases[1:]:
                send(base + here)

    x_starts = [sum(X_BLOCKS[:c]) for c in range(X_PARTS)]
    pieces = (
        [(routes, codes, None)]
        + [
            (tokens, x_all, pl.ds(x_starts[c] * LANES, X_BLOCKS[c] * LANES))
            for c in range(X_PARTS)
        ]
        + [
            (cotangent, dy_all, pl.ds(starts[c] * LANES, DY_BLOCKS[c] * LANES))
            for c in range(DY_PARTS)
        ]
    )

    def slot(p, s):
        _, dst, cols = pieces[p]
        if cols is None:
            return dst.at[s]
        return dst.at[pl.ds(s * rows, rows), cols]

    groups = [0] + [1] * X_PARTS + [2] * DY_PARTS

    def held_by(g, s):
        if g == 0:
            return codes.at[s]
        return (x_all, dy_all)[g - 1].at[pl.ds(s * rows, rows)]

    loads = [
        pltpu.make_async_copy(src, dst, local_sem.at[g])
        for g, (src, dst) in enumerate(
            (
                (routes, held_by(0, 0)),
                (tokens, held_by(1, 0)),
                (cotangent, held_by(2, 0)),
                (param_gu, gu_wide),
                (plan_in, plan),
            )
        )
    ]
    home = me % plane
    along_z = [((z + d) % zs) * plane + home for d in (1, zs - 1)]
    along_x = [me - x + (x + d) % X_SIZE for d in (1, X_SIZE - 1)]
    along_y = [me - y * X_SIZE + (1 - y) * X_SIZE]
    barrier = pltpu.get_barrier_semaphore()
    for other in (across, sibling):
        pl.semaphore_signal(barrier, inc=1, device_id={"expert": other}, device_id_type=MESH)
    for other in along_z + along_x + along_y:
        pl.semaphore_signal(barrier, inc=1, device_id={"node": other}, device_id_type=MESH)

    for load in loads:
        load.start()

    def down_load(b):
        cols = pl.ds(pl.multiple_of(b * LANES, LANES), LANES)
        dst = down_wide.at[pl.ds(pl.multiple_of(b * hid, hid), hid)]
        return pltpu.make_async_copy(param_down.at[:, cols], dst, local_sem.at[5])

    @pl.loop(0, width // LANES)
    def _(b):
        down_load(b).start()

    pl.semaphore_wait(barrier, 2 + len(along_z + along_x + along_y))

    def token_copy(src, dst, send_sem, recv_sem, other):
        return pltpu.make_async_remote_copy(
            src_ref=src,
            dst_ref=dst,
            send_sem=send_sem,
            recv_sem=recv_sem,
            device_id={"expert": other},
            device_id_type=MESH,
        )

    def to_sibling(p):
        g = groups[p]
        return token_copy(slot(p, 0), slot(p, 1), tok_send.at[0, g], beside_sem.at[g], sibling)

    def to_across(p):
        g = groups[p]
        return token_copy(slot(p, 0), slot(p, 2), tok_send.at[1, g], across_sem.at[p], across)

    def onward(p):
        g = groups[p]
        return token_copy(slot(p, 2), slot(p, 3), tok_send.at[2, g], onward_sem.at[p], sibling)

    def of_group(way, g):
        every = held_by(g, 1)
        return token_copy(every, every, tok_send.at[way, g], beside_sem.at[g], sibling)

    for p in range(len(pieces)):
        if groups.index(groups[p]) == p:
            loads[groups[p]].wait()
        to_across(p).start()
        to_sibling(p).start()

    rounds = [along_z] * (zs // 2) + [along_x] * (X_SIZE // 2) + [along_y]
    for r, others in enumerate(rounds):
        for other in others:
            pl.semaphore_signal(
                enter_sem.at[r], inc=1, device_id={"node": other}, device_id_type=MESH
            )
        pl.semaphore_wait(enter_sem.at[r], len(others))

    loads[3].wait()
    loads[4].wait()
    as_rows = pl.ds(0, hid * width // param_gu.shape[1])
    pltpu.make_async_copy(param_gu.at[as_rows], gu_wide.at[as_rows], local_sem.at[5]).wait()

    @pl.loop(0, width // TILE)
    def _(k):
        span = pl.ds(pl.multiple_of(k * TILE, TILE), TILE)
        gu_short[span, :] = gu_wide[span, :].astype(jnp.bfloat16)

    @pl.loop(0, width // LANES)
    def _(b):
        cols = pl.ds(pl.multiple_of(b * LANES, LANES), LANES)
        block = down_wide[pl.ds(pl.multiple_of(b * hid, hid), hid), :]
        down_short[:, cols] = block.astype(jnp.bfloat16)

    both[...] = jnp.zeros_like(both)
    dact[...] = jnp.zeros_like(dact)

    def arrive(p):
        to_across(p).wait_recv()
        onward(p).start()
        if groups.index(groups[p]) == p:
            of_group(0, groups[p]).wait_recv()
        onward(p).wait_recv()

    def turn(p):
        @pl.loop(x_starts[p] // 2, (x_starts[p] + X_BLOCKS[p]) // 2)
        def _(k):
            span = pl.ds(pl.multiple_of(k * 256, 256), 256)
            x_turned[span, :] = x_all[:, span].T

    arrive(0)
    for p in range(X_PARTS):
        arrive(1 + p)

        @pl.loop(x_starts[p] * LANES // TILE, (x_starts[p] + X_BLOCKS[p]) * LANES // TILE)
        def _(k):
            span = pl.ds(pl.multiple_of(k * TILE, TILE), TILE)
            both[...] += jnp.dot(
                x_all[:, span], gu_short[span, :], preferred_element_type=jnp.float32
            )

        if p < X_PARTS - 1:
            turn(p)

    def picked_at(s):
        named = codes[s]
        hit = jnp.where((named[0:1, :] == expert) | (named[1:2, :] == expert), 1, 0)
        return jnp.broadcast_to(hit, (rows, rows)).T != 0

    in_scale = 1.0 / math.sqrt(width)
    hid_scale = 1.0 / math.sqrt(hid)
    first = lax.broadcasted_iota(jnp.int32, (hid, hid), 0)
    second = lax.broadcasted_iota(jnp.int32, (hid, hid), 1)
    wanted = jnp.where(first < hid // 2, 2 * first, 2 * first - (hid - 1))
    order = jnp.where(second == wanted, 1.0, 0.0).astype(jnp.bfloat16)
    for s in range(experts):
        part = pl.ds(s * rows, rows)
        gate = both[part, :hid] * in_scale
        upper = both[part, hid:] * in_scale
        act = jnp.where(picked_at(s), gate * jax.nn.sigmoid(gate) * upper, 0.0)
        act_turned[:, part] = lax.dot_general(
            order,
            act.astype(jnp.bfloat16),
            (((1,), (1,)), ((), ())),
            preferred_element_type=jnp.float32,
        ).astype(jnp.bfloat16)

    def exchange(peer, src, dst, send_sem, recv_sem):
        return pltpu.make_async_remote_copy(
            src_ref=src,
            dst_ref=dst,
            send_sem=send_sem,
            recv_sem=recv_sem,
            device_id={"node": peer},
            device_id_type=MESH,
        )

    def gu_out(peer, c):
        src = send_gu.at[peer, pl.ds(c * gu_part, gu_part)]
        return exchange(peer, src, got_gu[c].at[me], link_sem.at[0], gu_in.at[c])

    def some(ref, first, count, sem):
        most = ref.at[pl.ds(first, count)]
        return exchange((me + 1) % nodes, most, most, sem, sem)

    def slices(count, values, sem):
        return some(x_turned, 0, count * values // x_turned.shape[1], sem)

    spot = z * X_SIZE + x
    over = along_y[0]

    def down_out(peer, c):
        return exchange(
            peer, send_down[c].at[peer], got_down[c].at[me], link_sem.at[1], down_in.at[c]
        )

    def down_relay(peer, c):
        other = peer - y * X_SIZE + (1 - y) * X_SIZE
        return exchange(
            peer, send_down[c].at[other], relay_down[c].at[spot], link_sem.at[2], relay_in.at[c]
        )

    def down_over(k, c):
        return exchange(
            over,
            relay_down[c].at[pl.ds(k * X_SIZE, X_SIZE)],
            got_down[c].at[pl.ds(k * plane + y * X_SIZE, X_SIZE)],
            link_sem.at[3],
            down_in.at[c],
        )

    def send_row(c):
        def both_ways(peer):
            down_out(peer, c).start()
            down_relay(peer, c).start()

        @pl.loop(1, X_SIZE)
        def _(k):
            both_ways(z_bases[0] + y * X_SIZE + (x + k) % X_SIZE)

        @pl.loop(0, X_SIZE)
        def _(k):
            here = y * X_SIZE + (x + k) % X_SIZE
            for base in z_bases[1:]:
                both_ways(base + here)

    for c in range(DY_PARTS):
        arrive(1 + X_PARTS + c)
        blocks = DY_BLOCKS[c]
        down_part = 2 * blocks

        @pl.loop(0, blocks * LANES // TILE)
        def _(k):
            at = pl.multiple_of(starts[c] * LANES + k * TILE, TILE)
            span = pl.ds(at, TILE)
            dact[...] += lax.dot_general(
                dy_all[:, span],
                down_short[:, span],
                (((1,), (1,)), ((), ())),
                preferred_element_type=jnp.float32,
            )
            grad = jnp.dot(act_turned[...], dy_all[:, span], preferred_element_type=jnp.float32)
            grad = grad * (0.5 * hid_scale)
            for r in range(2):
                for i in range(TILE // LANES):
                    block = starts[c] + k * (TILE // LANES) + i
                    old = down_wide[pl.ds(block * hid + r, nodes, stride=2), :]
                    new = old - grad[r * nodes : (r + 1) * nodes, i * LANES : (i + 1) * LANES]
                    row = r * blocks + k * (TILE // LANES) + i
                    stage[pl.ds(row, nodes, stride=down_part), :] = new

        @pl.loop(0, nodes)
        def _(n):
            span = pl.ds(pl.multiple_of(n * down_part, down_part), down_part)
            send_down[c][n] = stage[span, :].astype(jnp.bfloat16)

        send_row(c)
        got_down[c][me] = send_down[c][me]
        relay_down[c][spot] = send_down[c][over]
        if c == 1:
            turn(X_PARTS - 1)

    for s in range(experts):
        part = pl.ds(s * rows, rows)
        gate = both[part, :hid] * in_scale
        upper = both[part, hid:] * in_scale
        sigma = jax.nn.sigmoid(gate)
        da = dact[part, :] * hid_scale
        picked = picked_at(s)
        dgate = da * upper * sigma * (1.0 + gate * (1.0 - sigma))
        dupper = da * gate * sigma
        dboth[part, :hid] = jnp.where(picked, dgate, 0.0).astype(jnp.bfloat16)
        dboth[part, hid:] = jnp.where(picked, dupper, 0.0).astype(jnp.bfloat16)

    @pl.loop(0, zs)
    def _(j):
        zt = (z + (j % 2) * ((j + 1) // 2) + (1 - j % 2) * (zs - j // 2)) % zs
        at = pl.multiple_of(zt * (plane * gu_rows), plane * gu_rows)
        span = pl.ds(at, plane * gu_rows)
        grad = jnp.dot(x_turned[span, :], dboth[...], preferred_element_type=jnp.float32)
        new = gu_wide[span, :] - grad * (0.5 * in_scale)
        send_gu[pl.ds(zt * plane, plane)] = new.astype(jnp.bfloat16).reshape(
            plane, gu_rows, new.shape[1]
        )
        for k in range(plane):
            peer = zt * plane + in_plane(k)
            if k == 0:

                @pl.when(j > 0)
                def _():
                    gu_out(peer, 0).start()

            else:
                gu_out(peer, 0).start()

    for c in range(DY_PARTS):
        some(relay_down[c], 1, nodes // Y_LO - 1, relay_in.at[c]).wait_recv()

        @pl.loop(0, zs)
        def _(k):
            down_over(k, c).start()

    for c in range(1, GU_PARTS):

        each_peer(lambda peer: gu_out(peer, c).start())

    for c in range(GU_PARTS):
        got_gu[c][me] = send_gu[me, pl.ds(c * gu_part, gu_part)]

    def shift_at(i):
        exponent, shift = plan[i], jnp.int32(1)
        for e in range(1, SHIFTS):
            shift = jnp.where(exponent == e, jnp.int32(1 << e), shift)
        return shift

    s0, s1, s2, s3 = (shift_at(i) for i in range(ROUNDS))

    def filtered(got, half, done, mean):
        def wide(index):
            return got[lax.rem(index, nodes)].astype(jnp.float32)

        def early(n, total):
            own = wide(n)
            half[n] = (own + wide(n + s0)) + (wide(n + s1) + wide(n + s0 + s1))
            return total + own

        total = lax.fori_loop(0, nodes, early, jnp.zeros(half.shape[1:], jnp.float32), unroll=2)
        mean[...] = total * (1.0 / nodes)

        def late(n, carry):
            value = (half[n] + half[lax.rem(n + s2, nodes)]) + (
                half[lax.rem(n + s3, nodes)] + half[lax.rem(n + s2 + s3, nodes)]
            )
            done[n] = (value * (1.0 / 16.0)).astype(jnp.bfloat16)
            return carry

        lax.fori_loop(0, nodes, late, 0, unroll=2)

    def gu_home(peer, c):
        dst = out_gu.at[me, pl.ds(c * gu_part, gu_part)]
        return exchange(peer, done_gu.at[c, peer], dst, link_sem.at[4], home_sem.at[0])

    def down_home(peer, c):
        return exchange(
            peer, done_down[c].at[peer], home_down[c].at[me], link_sem.at[5], home_sem.at[1]
        )

    for c in range(DY_PARTS):
        some(got_down[c], 0, nodes - 1, down_in.at[c]).wait_recv()
        blocks = DY_BLOCKS[c]
        filtered(
            got_down[c],
            half_down.at[:, pl.ds(0, 2 * blocks)],
            done_down[c],
            mean_stage.at[pl.ds(0, 2 * blocks)],
        )
        for r in range(2):
            for i in range(blocks):
                at = (starts[c] + i) * LANES
                mean_down[r : r + 1, at : at + LANES] = mean_stage[
                    r * blocks + i : r * blocks + i + 1, :
                ]

        each_peer(lambda peer: down_home(peer, c).start())

        home_down[c][me] = done_down[c][me]

    for c in range(GU_PARTS):
        some(got_gu[c], 0, nodes - 1, gu_in.at[c]).wait_recv()
        filtered(
            got_gu[c], half_gu, done_gu.at[c], mean_gu.at[pl.ds(c * gu_part, gu_part)]
        )

        each_peer(lambda peer: gu_home(peer, c).start())

        out_gu[me, pl.ds(c * gu_part, gu_part)] = done_gu[c, me]

    gu_values, down_values = gu_rows * param_gu.shape[1], hid // nodes * width
    slices(nodes - 1, down_values, home_sem.at[1]).wait_recv()

    for c in range(DY_PARTS):
        blocks = DY_BLOCKS[c]
        down_part = 2 * blocks

        @pl.loop(0, nodes)
        def _(n):
            span = pl.ds(pl.multiple_of(n * down_part, down_part), down_part)
            stage[span, :] = home_down[c][n].astype(jnp.float32)

        for i in range(blocks):
            for r in range(2):
                row = r * blocks + i
                turned[pl.ds(i * hid + r, nodes, stride=2), :] = stage[
                    pl.ds(row, nodes, stride=down_part), :
                ]
            at = (starts[c] + i) * LANES
            out_down[:, at : at + LANES] = turned[
                i * hid : (i + 1) * hid, :
            ].astype(jnp.bfloat16)

    for g in range(3):
        for way in range(3):
            of_group(way, g).wait_send()
    slices(nodes - 1, gu_values, link_sem.at[0]).wait_send()
    slices(nodes // Y_LO - 1, down_values, link_sem.at[1]).wait_send()
    slices(nodes // Y_LO - 1, down_values, link_sem.at[2]).wait_send()
    slices(nodes // Y_LO, down_values, link_sem.at[3]).wait_send()
    slices(nodes - 1, gu_values, link_sem.at[4]).wait_send()
    slices(nodes - 1, down_values, link_sem.at[5]).wait_send()
    slices(nodes - 1, gu_values, home_sem.at[0]).wait_recv()


def put_out(*refs):
    sems, copies = refs[-1], []
    for i in range(4):
        pieces = 4 if refs[i].shape[0] % 64 == 0 else 1
        share = refs[i].shape[0] // pieces
        for k in range(pieces):
            span = pl.ds(k * share, share)
            copies.append(
                pltpu.make_async_copy(refs[i].at[span], refs[4 + i].at[span], sems.at[len(copies)])
            )
    for copy in copies:
        copy.start()
    for copy in copies:
        copy.wait()


def step(param_gu, param_down, tokens, cotangent, routes, plan):
    nodes = lax.axis_size("node")
    experts = lax.axis_size("expert")
    rows, width = tokens.shape
    cols = param_gu.shape[1]
    hid = param_down.shape[0]
    gu_rows = width // nodes
    down_part = 2 * max(DY_BLOCKS)
    pieces = X_PARTS + 1 + DY_PARTS
    inside = pl.BlockSpec(memory_space=pltpu.VMEM)
    outside = pl.BlockSpec(memory_space=pltpu.HBM)
    short, wide = jnp.bfloat16, jnp.float32

    def body(*refs):
        kernel_body(nodes, *refs)

    held = [
        pltpu.with_memory_space_constraint(a, pltpu.HBM)
        for a in (plan, routes.T, tokens, cotangent, param_gu, param_down)
    ]
    mixed_gu, mixed_down, mean_gu, mean_down = pl.pallas_call(
        body,
        out_shape=(
            jax.ShapeDtypeStruct((nodes, gu_rows, cols), short),
            jax.ShapeDtypeStruct((hid, width), short),
            jax.ShapeDtypeStruct((gu_rows, cols), wide),
            jax.ShapeDtypeStruct((hid // nodes, width), wide),
        ),
        in_specs=[outside] * 6,
        out_specs=(inside,) * 4,
        scratch_shapes=[
            pltpu.VMEM((experts * rows, width), short),
            pltpu.VMEM((experts * rows, width), short),
            pltpu.VMEM((width, experts * rows), short),
            pltpu.VMEM((width, cols), wide),
            pltpu.VMEM((hid * width // LANES, LANES), wide),
            pltpu.VMEM((width, cols), short),
            pltpu.VMEM((hid, width), short),
            pltpu.VMEM((experts * rows, cols), wide),
            pltpu.VMEM((experts * rows, hid), wide),
            pltpu.VMEM((hid, experts * rows), short),
            pltpu.VMEM((experts * rows, cols), short),
            pltpu.VMEM((experts, 2, rows), jnp.int32),
            pltpu.VMEM((nodes * down_part, LANES), wide),
            pltpu.VMEM((nodes * down_part, LANES), wide),
            pltpu.VMEM((down_part, LANES), wide),
            pltpu.SMEM((ROUNDS,), jnp.int32),
            pltpu.VMEM((nodes, gu_rows // GU_PARTS, cols), wide),
            pltpu.VMEM((nodes, down_part, LANES), wide),
            pltpu.VMEM((nodes, gu_rows, cols), short),
            pltpu.VMEM((GU_PARTS, nodes, gu_rows // GU_PARTS, cols), short),
            pltpu.SemaphoreType.REGULAR((nodes // (Y_LO * X_SIZE) // 2 + X_SIZE // 2 + 1,)),
            pltpu.SemaphoreType.DMA((6,)),
            pltpu.SemaphoreType.DMA((3, 3)),
            pltpu.SemaphoreType.DMA((3,)),
            pltpu.SemaphoreType.DMA((pieces,)),
            pltpu.SemaphoreType.DMA((pieces,)),
            pltpu.SemaphoreType.DMA((6,)),
            pltpu.SemaphoreType.DMA((GU_PARTS,)),
            pltpu.SemaphoreType.DMA((DY_PARTS,)),
            pltpu.SemaphoreType.DMA((DY_PARTS,)),
            pltpu.SemaphoreType.DMA((2,)),
        ]
        + [pltpu.VMEM((nodes, gu_rows // GU_PARTS, cols), short)] * GU_PARTS
        + [pltpu.VMEM((nodes, 2 * b, LANES), short) for b in DY_BLOCKS] * 4
        + [pltpu.VMEM((nodes // Y_LO, 2 * b, LANES), short) for b in DY_BLOCKS],
        compiler_params=pltpu.CompilerParams(
            collective_id=1, has_side_effects=True, vmem_limit_bytes=48 * 1024 * 1024
        ),
        name="expert_gossip",
    )(*held)

    results = (mixed_gu.reshape(width, cols), mixed_down, mean_gu, mean_down)
    return pl.pallas_call(
        put_out,
        out_shape=tuple(jax.ShapeDtypeStruct(a.shape, a.dtype) for a in results),
        in_specs=[inside] * 4,
        out_specs=(outside,) * 4,
        scratch_shapes=[pltpu.SemaphoreType.DMA((13,))],
        compiler_params=pltpu.CompilerParams(vmem_limit_bytes=1024 * 1024),
        name="put_out",
    )(*results)


def solution(mesh):
    both = P(("node", "expert"), None)
    split = P("node", "expert")
    return jax.shard_map(
        step,
        mesh=mesh,
        in_specs=(split, split, both, both, both, P()),
        out_specs=(split, split, split, split),
        check_vma=False,
    )
```

```python
import math

import jax
import jax.numpy as jnp
from jax import lax
from jax.experimental import pallas as pl
from jax.experimental.pallas import tpu as pltpu
from jax.sharding import PartitionSpec as P

MESH = pl.DeviceIdType.MESH
ROUNDS = 4
SHIFTS = 6
X_BLOCKS = (8, 8, 8, 4, 4)
X_PARTS = len(X_BLOCKS)
DY_BLOCKS = (4,) * 8
DY_PARTS = len(DY_BLOCKS)
GU_PARTS = 4
LANES = 128
TILE = 512
Y_LO, X_SIZE = 2, 4


def kernel_body(
    nodes,
    plan_in,
    routes,
    tokens,
    cotangent,
    param_gu,
    param_down,
    out_gu,
    out_down,
    mean_gu,
    mean_down,
    x_all,
    dy_all,
    x_turned,
    gu_wide,
    down_wide,
    gu_short,
    down_short,
    both,
    dact,
    act_turned,
    dboth,
    codes,
    stage,
    turned,
    mean_stage,
    plan,
    half_gu,
    half_down,
    send_gu,
    done_gu,
    enter_sem,
    local_sem,
    tok_send,
    beside_sem,
    across_sem,
    onward_sem,
    link_sem,
    gu_in,
    down_in,
    relay_in,
    home_sem,
    *landing,
):
    got_gu, downs = landing[:GU_PARTS], landing[GU_PARTS:]
    send_down, got_down, done_down, home_down, relay_down = (
        downs[i * DY_PARTS : (i + 1) * DY_PARTS] for i in range(5)
    )
    me = lax.axis_index("node")
    expert = lax.axis_index("expert")
    experts = lax.axis_size("expert")
    plane = Y_LO * X_SIZE
    zs = nodes // plane
    z, y, x = me // plane, (me // X_SIZE) % Y_LO, me % X_SIZE
    sibling = expert + 1 - 2 * (expert % 2)
    across = (expert + 2) % experts
    rows, width = tokens.shape
    hid = param_down.shape[0]
    gu_rows = send_gu.shape[1]
    gu_part = gu_rows // GU_PARTS
    starts = [sum(DY_BLOCKS[:c]) for c in range(DY_PARTS)]

    steps = [0, zs // 2] + [d for j in range(zs // 2 - 1, 0, -1) for d in (j, zs - j)]
    z_bases = [((z + d) % zs) * plane for d in steps]

    def in_plane(k):
        return ((y + k // X_SIZE) % Y_LO) * X_SIZE + (x + k % X_SIZE) % X_SIZE

    def each_peer(send):
        @pl.loop(1, plane)
        def _(k):
            send(z_bases[0] + in_plane(k))

        @pl.loop(0, plane)
        def _(k):
            here = in_plane(k)
            for base in z_bases[1:]:
                send(base + here)

    x_starts = [sum(X_BLOCKS[:c]) for c in range(X_PARTS)]
    pieces = (
        [(routes, codes, None)]
        + [
            (tokens, x_all, pl.ds(x_starts[c] * LANES, X_BLOCKS[c] * LANES))
            for c in range(X_PARTS)
        ]
        + [
            (cotangent, dy_all, pl.ds(starts[c] * LANES, DY_BLOCKS[c] * LANES))
            for c in range(DY_PARTS)
        ]
    )

    def slot(p, s):
        _, dst, cols = pieces[p]
        if cols is None:
            return dst.at[s]
        return dst.at[pl.ds(s * rows, rows), cols]

    groups = [0] + [1] * X_PARTS + [2] * DY_PARTS

    def held_by(g, s):
        if g == 0:
            return codes.at[s]
        return (x_all, dy_all)[g - 1].at[pl.ds(s * rows, rows)]

    loads = [
        pltpu.make_async_copy(src, dst, local_sem.at[g])
        for g, (src, dst) in enumerate(
            (
                (routes, held_by(0, 0)),
                (tokens, held_by(1, 0)),
                (cotangent, held_by(2, 0)),
                (param_gu, gu_wide),
                (plan_in, plan),
            )
        )
    ]
    home = me % plane
    along_z = [((z + d) % zs) * plane + home for d in (1, zs - 1)]
    along_x = [me - x + (x + d) % X_SIZE for d in (1, X_SIZE - 1)]
    along_y = [me - y * X_SIZE + (1 - y) * X_SIZE]
    barrier = pltpu.get_barrier_semaphore()
    for other in (across, sibling):
        pl.semaphore_signal(barrier, inc=1, device_id={"expert": other}, device_id_type=MESH)
    for other in along_z + along_x + along_y:
        pl.semaphore_signal(barrier, inc=1, device_id={"node": other}, device_id_type=MESH)

    for load in loads:
        load.start()

    def down_load(b):
        cols = pl.ds(pl.multiple_of(b * LANES, LANES), LANES)
        dst = down_wide.at[pl.ds(pl.multiple_of(b * hid, hid), hid)]
        return pltpu.make_async_copy(param_down.at[:, cols], dst, local_sem.at[5])

    @pl.loop(0, width // LANES)
    def _(b):
        down_load(b).start()

    pl.semaphore_wait(barrier, 2 + len(along_z + along_x + along_y))

    def token_copy(src, dst, send_sem, recv_sem, other):
        return pltpu.make_async_remote_copy(
            src_ref=src,
            dst_ref=dst,
            send_sem=send_sem,
            recv_sem=recv_sem,
            device_id={"expert": other},
            device_id_type=MESH,
        )

    def to_sibling(p):
        g = groups[p]
        return token_copy(slot(p, 0), slot(p, 1), tok_send.at[0, g], beside_sem.at[g], sibling)

    def to_across(p):
        g = groups[p]
        return token_copy(slot(p, 0), slot(p, 2), tok_send.at[1, g], across_sem.at[p], across)

    def onward(p):
        g = groups[p]
        return token_copy(slot(p, 2), slot(p, 3), tok_send.at[2, g], onward_sem.at[p], sibling)

    def of_group(way, g):
        every = held_by(g, 1)
        return token_copy(every, every, tok_send.at[way, g], beside_sem.at[g], sibling)

    for p in range(len(pieces)):
        if groups.index(groups[p]) == p:
            loads[groups[p]].wait()
        to_across(p).start()
        to_sibling(p).start()

    rounds = [along_z] * (zs // 2) + [along_x] * (X_SIZE // 2) + [along_y]
    for r, others in enumerate(rounds):
        for other in others:
            pl.semaphore_signal(
                enter_sem.at[r], inc=1, device_id={"node": other}, device_id_type=MESH
            )
        pl.semaphore_wait(enter_sem.at[r], len(others))

    loads[3].wait()
    loads[4].wait()
    as_rows = pl.ds(0, hid * width // param_gu.shape[1])
    pltpu.make_async_copy(param_gu.at[as_rows], gu_wide.at[as_rows], local_sem.at[5]).wait()

    @pl.loop(0, width // TILE)
    def _(k):
        span = pl.ds(pl.multiple_of(k * TILE, TILE), TILE)
        gu_short[span, :] = gu_wide[span, :].astype(jnp.bfloat16)

    @pl.loop(0, width // LANES)
    def _(b):
        cols = pl.ds(pl.multiple_of(b * LANES, LANES), LANES)
        block = down_wide[pl.ds(pl.multiple_of(b * hid, hid), hid), :]
        down_short[:, cols] = block.astype(jnp.bfloat16)

    both[...] = jnp.zeros_like(both)
    dact[...] = jnp.zeros_like(dact)

    def arrive(p):
        to_across(p).wait_recv()
        onward(p).start()
        if groups.index(groups[p]) == p:
            of_group(0, groups[p]).wait_recv()
        onward(p).wait_recv()

    def turn(p):
        @pl.loop(x_starts[p] // 2, (x_starts[p] + X_BLOCKS[p]) // 2)
        def _(k):
            span = pl.ds(pl.multiple_of(k * 256, 256), 256)
            x_turned[span, :] = x_all[:, span].T

    arrive(0)
    for p in range(X_PARTS):
        arrive(1 + p)

        @pl.loop(x_starts[p] * LANES // TILE, (x_starts[p] + X_BLOCKS[p]) * LANES // TILE)
        def _(k):
            span = pl.ds(pl.multiple_of(k * TILE, TILE), TILE)
            both[...] += jnp.dot(
                x_all[:, span], gu_short[span, :], preferred_element_type=jnp.float32
            )

        if p < X_PARTS - 1:
            turn(p)

    def picked_at(s):
        named = codes[s]
        hit = jnp.where((named[0:1, :] == expert) | (named[1:2, :] == expert), 1, 0)
        return jnp.broadcast_to(hit, (rows, rows)).T != 0

    in_scale = 1.0 / math.sqrt(width)
    hid_scale = 1.0 / math.sqrt(hid)
    first = lax.broadcasted_iota(jnp.int32, (hid, hid), 0)
    second = lax.broadcasted_iota(jnp.int32, (hid, hid), 1)
    wanted = jnp.where(first < hid // 2, 2 * first, 2 * first - (hid - 1))
    order = jnp.where(second == wanted, 1.0, 0.0).astype(jnp.bfloat16)
    for s in range(experts):
        part = pl.ds(s * rows, rows)
        gate = both[part, :hid] * in_scale
        upper = both[part, hid:] * in_scale
        act = jnp.where(picked_at(s), gate * jax.nn.sigmoid(gate) * upper, 0.0)
        act_turned[:, part] = lax.dot_general(
            order,
            act.astype(jnp.bfloat16),
            (((1,), (1,)), ((), ())),
            preferred_element_type=jnp.float32,
        ).astype(jnp.bfloat16)

    def exchange(peer, src, dst, send_sem, recv_sem):
        return pltpu.make_async_remote_copy(
            src_ref=src,
            dst_ref=dst,
            send_sem=send_sem,
            recv_sem=recv_sem,
            device_id={"node": peer},
            device_id_type=MESH,
        )

    def gu_out(peer, c):
        src = send_gu.at[peer, pl.ds(c * gu_part, gu_part)]
        return exchange(peer, src, got_gu[c].at[me], link_sem.at[0], gu_in.at[c])

    def some(ref, first, count, sem):
        most = ref.at[pl.ds(first, count)]
        return exchange((me + 1) % nodes, most, most, sem, sem)

    def slices(count, values, sem):
        return some(x_turned, 0, count * values // x_turned.shape[1], sem)

    spot = z * X_SIZE + x
    over = along_y[0]

    def down_out(peer, c):
        return exchange(
            peer, send_down[c].at[peer], got_down[c].at[me], link_sem.at[1], down_in.at[c]
        )

    def down_relay(peer, c):
        other = peer - y * X_SIZE + (1 - y) * X_SIZE
        return exchange(
            peer, send_down[c].at[other], relay_down[c].at[spot], link_sem.at[2], relay_in.at[c]
        )

    def down_over(k, c):
        return exchange(
            over,
            relay_down[c].at[pl.ds(k * X_SIZE, X_SIZE)],
            got_down[c].at[pl.ds(k * plane + y * X_SIZE, X_SIZE)],
            link_sem.at[3],
            down_in.at[c],
        )

    def send_row(c):
        def both_ways(peer):
            down_out(peer, c).start()
            down_relay(peer, c).start()

        @pl.loop(1, X_SIZE)
        def _(k):
            both_ways(z_bases[0] + y * X_SIZE + (x + k) % X_SIZE)

        @pl.loop(0, X_SIZE)
        def _(k):
            here = y * X_SIZE + (x + k) % X_SIZE
            for base in z_bases[1:]:
                both_ways(base + here)

    for c in range(DY_PARTS):
        arrive(1 + X_PARTS + c)
        blocks = DY_BLOCKS[c]
        down_part = 2 * blocks

        @pl.loop(0, blocks * LANES // TILE)
        def _(k):
            at = pl.multiple_of(starts[c] * LANES + k * TILE, TILE)
            span = pl.ds(at, TILE)
            dact[...] += lax.dot_general(
                dy_all[:, span],
                down_short[:, span],
                (((1,), (1,)), ((), ())),
                preferred_element_type=jnp.float32,
            )
            grad = jnp.dot(act_turned[...], dy_all[:, span], preferred_element_type=jnp.float32)
            grad = grad * (0.5 * hid_scale)
            for r in range(2):
                for i in range(TILE // LANES):
                    block = starts[c] + k * (TILE // LANES) + i
                    old = down_wide[pl.ds(block * hid + r, nodes, stride=2), :]
                    new = old - grad[r * nodes : (r + 1) * nodes, i * LANES : (i + 1) * LANES]
                    row = r * blocks + k * (TILE // LANES) + i
                    stage[pl.ds(row, nodes, stride=down_part), :] = new

        some_nodes = 16
        for n in range(0, nodes, some_nodes):
            block = stage[n * down_part : (n + some_nodes) * down_part, :]
            send_down[c][n : n + some_nodes] = block.reshape(
                some_nodes, down_part, LANES
            ).astype(jnp.bfloat16)

        send_row(c)
        got_down[c][me] = send_down[c][me]
        relay_down[c][spot] = send_down[c][over]
        if c == 1:
            turn(X_PARTS - 1)

    for s in range(experts):
        part = pl.ds(s * rows, rows)
        gate = both[part, :hid] * in_scale
        upper = both[part, hid:] * in_scale
        sigma = jax.nn.sigmoid(gate)
        da = dact[part, :] * hid_scale
        picked = picked_at(s)
        dgate = da * upper * sigma * (1.0 + gate * (1.0 - sigma))
        dupper = da * gate * sigma
        dboth[part, :hid] = jnp.where(picked, dgate, 0.0).astype(jnp.bfloat16)
        dboth[part, hid:] = jnp.where(picked, dupper, 0.0).astype(jnp.bfloat16)

    @pl.loop(0, zs)
    def _(j):
        zt = (z + zs // 2 + (1 - j % 2) * (j // 2) - (j % 2) * ((j + 1) // 2)) % zs
        at = pl.multiple_of(zt * (plane * gu_rows), plane * gu_rows)
        span = pl.ds(at, plane * gu_rows)
        grad = jnp.dot(x_turned[span, :], dboth[...], preferred_element_type=jnp.float32)
        new = gu_wide[span, :] - grad * (0.5 * in_scale)
        send_gu[pl.ds(zt * plane, plane)] = new.astype(jnp.bfloat16).reshape(
            plane, gu_rows, new.shape[1]
        )
        for k in range(plane):
            peer = zt * plane + in_plane(k)
            if k == 0:

                @pl.when(j < zs - 1)
                def _():
                    gu_out(peer, 0).start()

            else:
                gu_out(peer, 0).start()

    for c in range(DY_PARTS):
        some(relay_down[c], 1, nodes // Y_LO - 1, relay_in.at[c]).wait_recv()

        @pl.loop(0, zs)
        def _(k):
            down_over(k, c).start()

    for c in range(1, GU_PARTS):

        each_peer(lambda peer: gu_out(peer, c).start())

    for c in range(GU_PARTS):
        got_gu[c][me] = send_gu[me, pl.ds(c * gu_part, gu_part)]

    def shift_at(i):
        exponent, shift = plan[i], jnp.int32(1)
        for e in range(1, SHIFTS):
            shift = jnp.where(exponent == e, jnp.int32(1 << e), shift)
        return shift

    s0, s1, s2, s3 = (shift_at(i) for i in range(ROUNDS))

    def filtered(got, half, done, mean):
        def wide(index):
            return got[lax.rem(index, nodes)].astype(jnp.float32)

        def early(n, total):
            own = wide(n)
            half[n] = (own + wide(n + s0)) + (wide(n + s1) + wide(n + s0 + s1))
            return total + own

        total = lax.fori_loop(0, nodes, early, jnp.zeros(half.shape[1:], jnp.float32), unroll=2)
        mean[...] = total * (1.0 / nodes)

        def late(n, carry):
            value = (half[n] + half[lax.rem(n + s2, nodes)]) + (
                half[lax.rem(n + s3, nodes)] + half[lax.rem(n + s2 + s3, nodes)]
            )
            done[n] = (value * (1.0 / 16.0)).astype(jnp.bfloat16)
            return carry

        lax.fori_loop(0, nodes, late, 0, unroll=2)

    def gu_home(peer, c):
        dst = out_gu.at[me, pl.ds(c * gu_part, gu_part)]
        return exchange(peer, done_gu.at[c, peer], dst, link_sem.at[4], home_sem.at[0])

    def down_home(peer, c):
        return exchange(
            peer, done_down[c].at[peer], home_down[c].at[me], link_sem.at[5], home_sem.at[1]
        )

    for c in range(DY_PARTS):
        some(got_down[c], 0, nodes - 1, down_in.at[c]).wait_recv()
        blocks = DY_BLOCKS[c]
        filtered(
            got_down[c],
            half_down.at[:, pl.ds(0, 2 * blocks)],
            done_down[c],
            mean_stage.at[pl.ds(0, 2 * blocks)],
        )
        for r in range(2):
            for i in range(blocks):
                at = (starts[c] + i) * LANES
                mean_down[r : r + 1, at : at + LANES] = mean_stage[
                    r * blocks + i : r * blocks + i + 1, :
                ]

        each_peer(lambda peer: down_home(peer, c).start())

        home_down[c][me] = done_down[c][me]

    for c in range(GU_PARTS):
        some(got_gu[c], 0, nodes - 1, gu_in.at[c]).wait_recv()
        filtered(
            got_gu[c], half_gu, done_gu.at[c], mean_gu.at[pl.ds(c * gu_part, gu_part)]
        )

        each_peer(lambda peer: gu_home(peer, c).start())

        out_gu[me, pl.ds(c * gu_part, gu_part)] = done_gu[c, me]

    gu_values, down_values = gu_rows * param_gu.shape[1], hid // nodes * width
    slices(nodes - 1, down_values, home_sem.at[1]).wait_recv()

    for c in range(DY_PARTS):
        blocks = DY_BLOCKS[c]
        down_part = 2 * blocks

        @pl.loop(0, nodes)
        def _(n):
            span = pl.ds(pl.multiple_of(n * down_part, down_part), down_part)
            stage[span, :] = home_down[c][n].astype(jnp.float32)

        for i in range(blocks):
            for r in range(2):
                row = r * blocks + i
                turned[pl.ds(i * hid + r, nodes, stride=2), :] = stage[
                    pl.ds(row, nodes, stride=down_part), :
                ]
            at = (starts[c] + i) * LANES
            out_down[:, at : at + LANES] = turned[
                i * hid : (i + 1) * hid, :
            ].astype(jnp.bfloat16)

    for g in range(3):
        for way in range(3):
            of_group(way, g).wait_send()
    slices(nodes - 1, gu_values, link_sem.at[0]).wait_send()
    slices(nodes // Y_LO - 1, down_values, link_sem.at[1]).wait_send()
    slices(nodes // Y_LO - 1, down_values, link_sem.at[2]).wait_send()
    slices(nodes // Y_LO, down_values, link_sem.at[3]).wait_send()
    slices(nodes - 1, gu_values, link_sem.at[4]).wait_send()
    slices(nodes - 1, down_values, link_sem.at[5]).wait_send()
    slices(nodes - 1, gu_values, home_sem.at[0]).wait_recv()


def put_out(*refs):
    sems, copies = refs[-1], []
    for i in range(4):
        pieces = 4 if refs[i].shape[0] % 64 == 0 else 1
        share = refs[i].shape[0] // pieces
        for k in range(pieces):
            span = pl.ds(k * share, share)
            copies.append(
                pltpu.make_async_copy(refs[i].at[span], refs[4 + i].at[span], sems.at[len(copies)])
            )
    for copy in copies:
        copy.start()
    for copy in copies:
        copy.wait()


def step(param_gu, param_down, tokens, cotangent, routes, plan):
    nodes = lax.axis_size("node")
    experts = lax.axis_size("expert")
    rows, width = tokens.shape
    cols = param_gu.shape[1]
    hid = param_down.shape[0]
    gu_rows = width // nodes
    down_part = 2 * max(DY_BLOCKS)
    pieces = X_PARTS + 1 + DY_PARTS
    inside = pl.BlockSpec(memory_space=pltpu.VMEM)
    outside = pl.BlockSpec(memory_space=pltpu.HBM)
    short, wide = jnp.bfloat16, jnp.float32

    def body(*refs):
        kernel_body(nodes, *refs)

    held = [
        pltpu.with_memory_space_constraint(a, pltpu.HBM)
        for a in (plan, routes.T, tokens, cotangent, param_gu, param_down)
    ]
    mixed_gu, mixed_down, mean_gu, mean_down = pl.pallas_call(
        body,
        out_shape=(
            jax.ShapeDtypeStruct((nodes, gu_rows, cols), short),
            jax.ShapeDtypeStruct((hid, width), short),
            jax.ShapeDtypeStruct((gu_rows, cols), wide),
            jax.ShapeDtypeStruct((hid // nodes, width), wide),
        ),
        in_specs=[outside] * 6,
        out_specs=(inside,) * 4,
        scratch_shapes=[
            pltpu.VMEM((experts * rows, width), short),
            pltpu.VMEM((experts * rows, width), short),
            pltpu.VMEM((width, experts * rows), short),
            pltpu.VMEM((width, cols), wide),
            pltpu.VMEM((hid * width // LANES, LANES), wide),
            pltpu.VMEM((width, cols), short),
            pltpu.VMEM((hid, width), short),
            pltpu.VMEM((experts * rows, cols), wide),
            pltpu.VMEM((experts * rows, hid), wide),
            pltpu.VMEM((hid, experts * rows), short),
            pltpu.VMEM((experts * rows, cols), short),
            pltpu.VMEM((experts, 2, rows), jnp.int32),
            pltpu.VMEM((nodes * down_part, LANES), wide),
            pltpu.VMEM((nodes * down_part, LANES), wide),
            pltpu.VMEM((down_part, LANES), wide),
            pltpu.SMEM((ROUNDS,), jnp.int32),
            pltpu.VMEM((nodes, gu_rows // GU_PARTS, cols), wide),
            pltpu.VMEM((nodes, down_part, LANES), wide),
            pltpu.VMEM((nodes, gu_rows, cols), short),
            pltpu.VMEM((GU_PARTS, nodes, gu_rows // GU_PARTS, cols), short),
            pltpu.SemaphoreType.REGULAR((nodes // (Y_LO * X_SIZE) // 2 + X_SIZE // 2 + 1,)),
            pltpu.SemaphoreType.DMA((6,)),
            pltpu.SemaphoreType.DMA((3, 3)),
            pltpu.SemaphoreType.DMA((3,)),
            pltpu.SemaphoreType.DMA((pieces,)),
            pltpu.SemaphoreType.DMA((pieces,)),
            pltpu.SemaphoreType.DMA((6,)),
            pltpu.SemaphoreType.DMA((GU_PARTS,)),
            pltpu.SemaphoreType.DMA((DY_PARTS,)),
            pltpu.SemaphoreType.DMA((DY_PARTS,)),
            pltpu.SemaphoreType.DMA((2,)),
        ]
        + [pltpu.VMEM((nodes, gu_rows // GU_PARTS, cols), short)] * GU_PARTS
        + [pltpu.VMEM((nodes, 2 * b, LANES), short) for b in DY_BLOCKS] * 4
        + [pltpu.VMEM((nodes // Y_LO, 2 * b, LANES), short) for b in DY_BLOCKS],
        compiler_params=pltpu.CompilerParams(
            collective_id=1, has_side_effects=True, vmem_limit_bytes=48 * 1024 * 1024
        ),
        name="expert_gossip",
    )(*held)

    results = (mixed_gu.reshape(width, cols), mixed_down, mean_gu, mean_down)
    return pl.pallas_call(
        put_out,
        out_shape=tuple(jax.ShapeDtypeStruct(a.shape, a.dtype) for a in results),
        in_specs=[inside] * 4,
        out_specs=(outside,) * 4,
        scratch_shapes=[pltpu.SemaphoreType.DMA((13,))],
        compiler_params=pltpu.CompilerParams(vmem_limit_bytes=1024 * 1024),
        name="put_out",
    )(*results)


def solution(mesh):
    both = P(("node", "expert"), None)
    split = P("node", "expert")
    return jax.shard_map(
        step,
        mesh=mesh,
        in_specs=(split, split, both, both, both, P()),
        out_specs=(split, split, split, split),
        check_vma=False,
    )
```

```python
import math

import jax
import jax.numpy as jnp
from jax import lax
from jax.experimental import pallas as pl
from jax.experimental.pallas import tpu as pltpu
from jax.sharding import PartitionSpec as P

MESH = pl.DeviceIdType.MESH
ROUNDS = 4
SHIFTS = 6
X_BLOCKS = (8, 8, 8, 4, 4)
X_PARTS = len(X_BLOCKS)
DY_BLOCKS = (4,) * 8
DY_PARTS = len(DY_BLOCKS)
GU_PARTS = 4
LANES = 128
TILE = 512
Y_LO, X_SIZE = 2, 4


def kernel_body(
    nodes,
    plan_in,
    routes,
    tokens,
    cotangent,
    param_gu,
    param_down,
    out_gu,
    out_down,
    mean_gu,
    mean_down,
    x_all,
    dy_all,
    x_turned,
    gu_wide,
    down_wide,
    gu_short,
    down_short,
    both,
    dact,
    act_turned,
    dboth,
    codes,
    stage,
    turned,
    mean_stage,
    plan,
    half_gu,
    half_down,
    send_gu,
    done_gu,
    enter_sem,
    local_sem,
    tok_send,
    beside_sem,
    across_sem,
    onward_sem,
    link_sem,
    gu_in,
    down_in,
    relay_in,
    home_sem,
    *landing,
):
    got_gu, downs = landing[:GU_PARTS], landing[GU_PARTS:]
    send_down, got_down, done_down, home_down, relay_down = (
        downs[i * DY_PARTS : (i + 1) * DY_PARTS] for i in range(5)
    )
    me = lax.axis_index("node")
    expert = lax.axis_index("expert")
    experts = lax.axis_size("expert")
    plane = Y_LO * X_SIZE
    zs = nodes // plane
    z, y, x = me // plane, (me // X_SIZE) % Y_LO, me % X_SIZE
    sibling = expert + 1 - 2 * (expert % 2)
    across = (expert + 2) % experts
    rows, width = tokens.shape
    hid = param_down.shape[0]
    gu_rows = send_gu.shape[1]
    gu_part = gu_rows // GU_PARTS
    starts = [sum(DY_BLOCKS[:c]) for c in range(DY_PARTS)]

    steps = [0, zs // 2] + [d for j in range(zs // 2 - 1, 0, -1) for d in (j, zs - j)]
    z_bases = [((z + d) % zs) * plane for d in steps]

    def in_plane(k):
        return ((y + k // X_SIZE) % Y_LO) * X_SIZE + (x + k % X_SIZE) % X_SIZE

    def each_peer(send):
        @pl.loop(1, plane)
        def _(k):
            send(z_bases[0] + in_plane(k))

        @pl.loop(0, plane)
        def _(k):
            here = in_plane(k)
            for base in z_bases[1:]:
                send(base + here)

    x_starts = [sum(X_BLOCKS[:c]) for c in range(X_PARTS)]
    pieces = (
        [(routes, codes, None)]
        + [
            (tokens, x_all, pl.ds(x_starts[c] * LANES, X_BLOCKS[c] * LANES))
            for c in range(X_PARTS)
        ]
        + [
            (cotangent, dy_all, pl.ds(starts[c] * LANES, DY_BLOCKS[c] * LANES))
            for c in range(DY_PARTS)
        ]
    )

    def slot(p, s):
        _, dst, cols = pieces[p]
        if cols is None:
            return dst.at[s]
        return dst.at[pl.ds(s * rows, rows), cols]

    groups = [0] + [1] * X_PARTS + [2] * DY_PARTS

    def held_by(g, s):
        if g == 0:
            return codes.at[s]
        return (x_all, dy_all)[g - 1].at[pl.ds(s * rows, rows)]

    loads = [
        pltpu.make_async_copy(src, dst, local_sem.at[g])
        for g, (src, dst) in enumerate(
            (
                (routes, held_by(0, 0)),
                (tokens, held_by(1, 0)),
                (cotangent, held_by(2, 0)),
                (param_gu, gu_wide),
                (plan_in, plan),
            )
        )
    ]
    home = me % plane
    along_z = [((z + d) % zs) * plane + home for d in (1, zs - 1)]
    along_x = [me - x + (x + d) % X_SIZE for d in (1, X_SIZE - 1)]
    along_y = [me - y * X_SIZE + (1 - y) * X_SIZE]
    barrier = pltpu.get_barrier_semaphore()
    for other in (across, sibling):
        pl.semaphore_signal(barrier, inc=1, device_id={"expert": other}, device_id_type=MESH)
    for other in along_z + along_x + along_y:
        pl.semaphore_signal(barrier, inc=1, device_id={"node": other}, device_id_type=MESH)

    for load in loads:
        load.start()

    def down_load(b):
        cols = pl.ds(pl.multiple_of(b * LANES, LANES), LANES)
        dst = down_wide.at[pl.ds(pl.multiple_of(b * hid, hid), hid)]
        return pltpu.make_async_copy(param_down.at[:, cols], dst, local_sem.at[5])

    @pl.loop(0, width // LANES)
    def _(b):
        down_load(b).start()

    pl.semaphore_wait(barrier, 2 + len(along_z + along_x + along_y))

    def token_copy(src, dst, send_sem, recv_sem, other):
        return pltpu.make_async_remote_copy(
            src_ref=src,
            dst_ref=dst,
            send_sem=send_sem,
            recv_sem=recv_sem,
            device_id={"expert": other},
            device_id_type=MESH,
        )

    def to_sibling(p):
        g = groups[p]
        return token_copy(slot(p, 0), slot(p, 1), tok_send.at[0, g], beside_sem.at[g], sibling)

    def to_across(p):
        g = groups[p]
        return token_copy(slot(p, 0), slot(p, 2), tok_send.at[1, g], across_sem.at[p], across)

    def onward(p):
        g = groups[p]
        return token_copy(slot(p, 2), slot(p, 3), tok_send.at[2, g], onward_sem.at[p], sibling)

    def of_group(way, g):
        every = held_by(g, 1)
        return token_copy(every, every, tok_send.at[way, g], beside_sem.at[g], sibling)

    for p in range(len(pieces)):
        if groups.index(groups[p]) == p:
            loads[groups[p]].wait()
        to_across(p).start()
        to_sibling(p).start()

    rounds = [along_z] * (zs // 2) + [along_x] * (X_SIZE // 2) + [along_y]
    for r, others in enumerate(rounds):
        for other in others:
            pl.semaphore_signal(
                enter_sem.at[r], inc=1, device_id={"node": other}, device_id_type=MESH
            )
        pl.semaphore_wait(enter_sem.at[r], len(others))

    loads[3].wait()
    loads[4].wait()
    as_rows = pl.ds(0, hid * width // param_gu.shape[1])
    pltpu.make_async_copy(param_gu.at[as_rows], gu_wide.at[as_rows], local_sem.at[5]).wait()

    @pl.loop(0, width // TILE)
    def _(k):
        span = pl.ds(pl.multiple_of(k * TILE, TILE), TILE)
        gu_short[span, :] = gu_wide[span, :].astype(jnp.bfloat16)

    @pl.loop(0, width // LANES)
    def _(b):
        cols = pl.ds(pl.multiple_of(b * LANES, LANES), LANES)
        block = down_wide[pl.ds(pl.multiple_of(b * hid, hid), hid), :]
        down_short[:, cols] = block.astype(jnp.bfloat16)

    both[...] = jnp.zeros_like(both)
    dact[...] = jnp.zeros_like(dact)

    def arrive(p):
        to_across(p).wait_recv()
        onward(p).start()
        if groups.index(groups[p]) == p:
            of_group(0, groups[p]).wait_recv()
        onward(p).wait_recv()

    def turn(p):
        @pl.loop(x_starts[p] // 2, (x_starts[p] + X_BLOCKS[p]) // 2)
        def _(k):
            span = pl.ds(pl.multiple_of(k * 256, 256), 256)
            x_turned[span, :] = x_all[:, span].T

    arrive(0)
    for p in range(X_PARTS):
        arrive(1 + p)

        @pl.loop(x_starts[p] * LANES // TILE, (x_starts[p] + X_BLOCKS[p]) * LANES // TILE)
        def _(k):
            span = pl.ds(pl.multiple_of(k * TILE, TILE), TILE)
            both[...] += jnp.dot(
                x_all[:, span], gu_short[span, :], preferred_element_type=jnp.float32
            )

        if p < X_PARTS - 1:
            turn(p)

    def picked_at(s):
        named = codes[s]
        hit = jnp.where((named[0:1, :] == expert) | (named[1:2, :] == expert), 1, 0)
        return jnp.broadcast_to(hit, (rows, rows)).T != 0

    in_scale = 1.0 / math.sqrt(width)
    hid_scale = 1.0 / math.sqrt(hid)
    first = lax.broadcasted_iota(jnp.int32, (hid, hid), 0)
    second = lax.broadcasted_iota(jnp.int32, (hid, hid), 1)
    wanted = jnp.where(first < hid // 2, 2 * first, 2 * first - (hid - 1))
    order = jnp.where(second == wanted, 1.0, 0.0).astype(jnp.bfloat16)
    for s in range(experts):
        part = pl.ds(s * rows, rows)
        gate = both[part, :hid] * in_scale
        upper = both[part, hid:] * in_scale
        act = jnp.where(picked_at(s), gate * jax.nn.sigmoid(gate) * upper, 0.0)
        act_turned[:, part] = lax.dot_general(
            order,
            act.astype(jnp.bfloat16),
            (((1,), (1,)), ((), ())),
            preferred_element_type=jnp.float32,
        ).astype(jnp.bfloat16)

    def exchange(peer, src, dst, send_sem, recv_sem):
        return pltpu.make_async_remote_copy(
            src_ref=src,
            dst_ref=dst,
            send_sem=send_sem,
            recv_sem=recv_sem,
            device_id={"node": peer},
            device_id_type=MESH,
        )

    def gu_out(peer, c):
        src = send_gu.at[peer, pl.ds(c * gu_part, gu_part)]
        return exchange(peer, src, got_gu[c].at[me], link_sem.at[0], gu_in.at[c])

    def some(ref, first, count, sem):
        most = ref.at[pl.ds(first, count)]
        return exchange((me + 1) % nodes, most, most, sem, sem)

    def slices(count, values, sem):
        return some(x_turned, 0, count * values // x_turned.shape[1], sem)

    spot = z * X_SIZE + x
    over = along_y[0]

    def down_out(peer, c):
        return exchange(
            peer, send_down[c].at[peer], got_down[c].at[me], link_sem.at[1], down_in.at[c]
        )

    def down_relay(peer, c):
        other = peer - y * X_SIZE + (1 - y) * X_SIZE
        return exchange(
            peer, send_down[c].at[other], relay_down[c].at[spot], link_sem.at[2], relay_in.at[c]
        )

    def down_over(k, c):
        return exchange(
            over,
            relay_down[c].at[pl.ds(k * X_SIZE, X_SIZE)],
            got_down[c].at[pl.ds(k * plane + y * X_SIZE, X_SIZE)],
            link_sem.at[3],
            down_in.at[c],
        )

    def send_row(c):
        def both_ways(peer):
            down_out(peer, c).start()
            down_relay(peer, c).start()

        @pl.loop(1, X_SIZE)
        def _(k):
            both_ways(z_bases[0] + y * X_SIZE + (x + k) % X_SIZE)

        @pl.loop(0, X_SIZE)
        def _(k):
            here = y * X_SIZE + (x + k) % X_SIZE
            for base in z_bases[1:]:
                both_ways(base + here)

    def add_dact(c):
        @pl.loop(0, DY_BLOCKS[c] * LANES // TILE)
        def _(k):
            span = pl.ds(pl.multiple_of(starts[c] * LANES + k * TILE, TILE), TILE)
            dact[...] += lax.dot_general(
                dy_all[:, span],
                down_short[:, span],
                (((1,), (1,)), ((), ())),
                preferred_element_type=jnp.float32,
            )

    for c in range(DY_PARTS):
        arrive(1 + X_PARTS + c)
        if c == DY_PARTS - 1:
            add_dact(c)
        blocks = DY_BLOCKS[c]
        down_part = 2 * blocks

        @pl.loop(0, blocks * LANES // TILE)
        def _(k):
            at = pl.multiple_of(starts[c] * LANES + k * TILE, TILE)
            span = pl.ds(at, TILE)
            grad = jnp.dot(act_turned[...], dy_all[:, span], preferred_element_type=jnp.float32)
            grad = grad * (0.5 * hid_scale)
            for r in range(2):
                for i in range(TILE // LANES):
                    block = starts[c] + k * (TILE // LANES) + i
                    old = down_wide[pl.ds(block * hid + r, nodes, stride=2), :]
                    new = old - grad[r * nodes : (r + 1) * nodes, i * LANES : (i + 1) * LANES]
                    row = r * blocks + k * (TILE // LANES) + i
                    stage[pl.ds(row, nodes, stride=down_part), :] = new

        some_nodes = 16
        for n in range(0, nodes, some_nodes):
            block = stage[n * down_part : (n + some_nodes) * down_part, :]
            send_down[c][n : n + some_nodes] = block.reshape(
                some_nodes, down_part, LANES
            ).astype(jnp.bfloat16)

        send_row(c)
        if c < DY_PARTS - 1:
            add_dact(c)
        got_down[c][me] = send_down[c][me]
        relay_down[c][spot] = send_down[c][over]
        if c == 1:
            turn(X_PARTS - 1)

    for s in range(experts):
        part = pl.ds(s * rows, rows)
        gate = both[part, :hid] * in_scale
        upper = both[part, hid:] * in_scale
        sigma = jax.nn.sigmoid(gate)
        da = dact[part, :] * hid_scale
        picked = picked_at(s)
        dgate = da * upper * sigma * (1.0 + gate * (1.0 - sigma))
        dupper = da * gate * sigma
        dboth[part, :hid] = jnp.where(picked, dgate, 0.0).astype(jnp.bfloat16)
        dboth[part, hid:] = jnp.where(picked, dupper, 0.0).astype(jnp.bfloat16)

    @pl.loop(0, zs)
    def _(j):
        zt = (z + zs // 2 + (1 - j % 2) * (j // 2) - (j % 2) * ((j + 1) // 2)) % zs
        at = pl.multiple_of(zt * (plane * gu_rows), plane * gu_rows)
        span = pl.ds(at, plane * gu_rows)
        grad = jnp.dot(x_turned[span, :], dboth[...], preferred_element_type=jnp.float32)
        new = gu_wide[span, :] - grad * (0.5 * in_scale)
        send_gu[pl.ds(zt * plane, plane)] = new.astype(jnp.bfloat16).reshape(
            plane, gu_rows, new.shape[1]
        )
        for k in range(plane):
            peer = zt * plane + in_plane(k)
            if k == 0:

                @pl.when(j < zs - 1)
                def _():
                    gu_out(peer, 0).start()

            else:
                gu_out(peer, 0).start()

    for c in range(DY_PARTS):
        some(relay_down[c], 1, nodes // Y_LO - 1, relay_in.at[c]).wait_recv()

        @pl.loop(0, zs)
        def _(k):
            down_over(k, c).start()

    for c in range(1, GU_PARTS):

        each_peer(lambda peer: gu_out(peer, c).start())

    for c in range(GU_PARTS):
        got_gu[c][me] = send_gu[me, pl.ds(c * gu_part, gu_part)]

    def shift_at(i):
        exponent, shift = plan[i], jnp.int32(1)
        for e in range(1, SHIFTS):
            shift = jnp.where(exponent == e, jnp.int32(1 << e), shift)
        return shift

    s0, s1, s2, s3 = (shift_at(i) for i in range(ROUNDS))

    def filtered(got, half, done, mean):
        def wide(index):
            return got[lax.rem(index, nodes)].astype(jnp.float32)

        def early(n, total):
            own = wide(n)
            half[n] = (own + wide(n + s0)) + (wide(n + s1) + wide(n + s0 + s1))
            return total + own

        total = lax.fori_loop(0, nodes, early, jnp.zeros(half.shape[1:], jnp.float32), unroll=2)
        mean[...] = total * (1.0 / nodes)

        def late(n, carry):
            value = (half[n] + half[lax.rem(n + s2, nodes)]) + (
                half[lax.rem(n + s3, nodes)] + half[lax.rem(n + s2 + s3, nodes)]
            )
            done[n] = (value * (1.0 / 16.0)).astype(jnp.bfloat16)
            return carry

        lax.fori_loop(0, nodes, late, 0, unroll=2)

    def gu_home(peer, c):
        dst = out_gu.at[me, pl.ds(c * gu_part, gu_part)]
        return exchange(peer, done_gu.at[c, peer], dst, link_sem.at[4], home_sem.at[0])

    def down_home(peer, c):
        return exchange(
            peer, done_down[c].at[peer], home_down[c].at[me], link_sem.at[5], home_sem.at[1]
        )

    for c in range(DY_PARTS):
        some(got_down[c], 0, nodes - 1, down_in.at[c]).wait_recv()
        blocks = DY_BLOCKS[c]
        filtered(
            got_down[c],
            half_down.at[:, pl.ds(0, 2 * blocks)],
            done_down[c],
            mean_stage.at[pl.ds(0, 2 * blocks)],
        )
        for r in range(2):
            for i in range(blocks):
                at = (starts[c] + i) * LANES
                mean_down[r : r + 1, at : at + LANES] = mean_stage[
                    r * blocks + i : r * blocks + i + 1, :
                ]

        each_peer(lambda peer: down_home(peer, c).start())

        home_down[c][me] = done_down[c][me]

    for c in range(GU_PARTS):
        some(got_gu[c], 0, nodes - 1, gu_in.at[c]).wait_recv()
        filtered(
            got_gu[c], half_gu, done_gu.at[c], mean_gu.at[pl.ds(c * gu_part, gu_part)]
        )

        each_peer(lambda peer: gu_home(peer, c).start())

        out_gu[me, pl.ds(c * gu_part, gu_part)] = done_gu[c, me]

    gu_values, down_values = gu_rows * param_gu.shape[1], hid // nodes * width
    slices(nodes - 1, down_values, home_sem.at[1]).wait_recv()

    for c in range(DY_PARTS):
        blocks = DY_BLOCKS[c]
        down_part = 2 * blocks

        @pl.loop(0, nodes)
        def _(n):
            span = pl.ds(pl.multiple_of(n * down_part, down_part), down_part)
            stage[span, :] = home_down[c][n].astype(jnp.float32)

        for i in range(blocks):
            for r in range(2):
                row = r * blocks + i
                turned[pl.ds(i * hid + r, nodes, stride=2), :] = stage[
                    pl.ds(row, nodes, stride=down_part), :
                ]
            at = (starts[c] + i) * LANES
            out_down[:, at : at + LANES] = turned[
                i * hid : (i + 1) * hid, :
            ].astype(jnp.bfloat16)

    for g in range(3):
        for way in range(3):
            of_group(way, g).wait_send()
    slices(nodes - 1, gu_values, link_sem.at[0]).wait_send()
    slices(nodes // Y_LO - 1, down_values, link_sem.at[1]).wait_send()
    slices(nodes // Y_LO - 1, down_values, link_sem.at[2]).wait_send()
    slices(nodes // Y_LO, down_values, link_sem.at[3]).wait_send()
    slices(nodes - 1, gu_values, link_sem.at[4]).wait_send()
    slices(nodes - 1, down_values, link_sem.at[5]).wait_send()
    slices(nodes - 1, gu_values, home_sem.at[0]).wait_recv()


def put_out(*refs):
    sems, copies = refs[-1], []
    for i in range(4):
        pieces = 4 if refs[i].shape[0] % 64 == 0 else 1
        share = refs[i].shape[0] // pieces
        for k in range(pieces):
            span = pl.ds(k * share, share)
            copies.append(
                pltpu.make_async_copy(refs[i].at[span], refs[4 + i].at[span], sems.at[len(copies)])
            )
    for copy in copies:
        copy.start()
    for copy in copies:
        copy.wait()


def step(param_gu, param_down, tokens, cotangent, routes, plan):
    nodes = lax.axis_size("node")
    experts = lax.axis_size("expert")
    rows, width = tokens.shape
    cols = param_gu.shape[1]
    hid = param_down.shape[0]
    gu_rows = width // nodes
    down_part = 2 * max(DY_BLOCKS)
    pieces = X_PARTS + 1 + DY_PARTS
    inside = pl.BlockSpec(memory_space=pltpu.VMEM)
    outside = pl.BlockSpec(memory_space=pltpu.HBM)
    short, wide = jnp.bfloat16, jnp.float32

    def body(*refs):
        kernel_body(nodes, *refs)

    held = [
        pltpu.with_memory_space_constraint(a, pltpu.HBM)
        for a in (plan, routes.T, tokens, cotangent, param_gu, param_down)
    ]
    mixed_gu, mixed_down, mean_gu, mean_down = pl.pallas_call(
        body,
        out_shape=(
            jax.ShapeDtypeStruct((nodes, gu_rows, cols), short),
            jax.ShapeDtypeStruct((hid, width), short),
            jax.ShapeDtypeStruct((gu_rows, cols), wide),
            jax.ShapeDtypeStruct((hid // nodes, width), wide),
        ),
        in_specs=[outside] * 6,
        out_specs=(inside,) * 4,
        scratch_shapes=[
            pltpu.VMEM((experts * rows, width), short),
            pltpu.VMEM((experts * rows, width), short),
            pltpu.VMEM((width, experts * rows), short),
            pltpu.VMEM((width, cols), wide),
            pltpu.VMEM((hid * width // LANES, LANES), wide),
            pltpu.VMEM((width, cols), short),
            pltpu.VMEM((hid, width), short),
            pltpu.VMEM((experts * rows, cols), wide),
            pltpu.VMEM((experts * rows, hid), wide),
            pltpu.VMEM((hid, experts * rows), short),
            pltpu.VMEM((experts * rows, cols), short),
            pltpu.VMEM((experts, 2, rows), jnp.int32),
            pltpu.VMEM((nodes * down_part, LANES), wide),
            pltpu.VMEM((nodes * down_part, LANES), wide),
            pltpu.VMEM((down_part, LANES), wide),
            pltpu.SMEM((ROUNDS,), jnp.int32),
            pltpu.VMEM((nodes, gu_rows // GU_PARTS, cols), wide),
            pltpu.VMEM((nodes, down_part, LANES), wide),
            pltpu.VMEM((nodes, gu_rows, cols), short),
            pltpu.VMEM((GU_PARTS, nodes, gu_rows // GU_PARTS, cols), short),
            pltpu.SemaphoreType.REGULAR((nodes // (Y_LO * X_SIZE) // 2 + X_SIZE // 2 + 1,)),
            pltpu.SemaphoreType.DMA((6,)),
            pltpu.SemaphoreType.DMA((3, 3)),
            pltpu.SemaphoreType.DMA((3,)),
            pltpu.SemaphoreType.DMA((pieces,)),
            pltpu.SemaphoreType.DMA((pieces,)),
            pltpu.SemaphoreType.DMA((6,)),
            pltpu.SemaphoreType.DMA((GU_PARTS,)),
            pltpu.SemaphoreType.DMA((DY_PARTS,)),
            pltpu.SemaphoreType.DMA((DY_PARTS,)),
            pltpu.SemaphoreType.DMA((2,)),
        ]
        + [pltpu.VMEM((nodes, gu_rows // GU_PARTS, cols), short)] * GU_PARTS
        + [pltpu.VMEM((nodes, 2 * b, LANES), short) for b in DY_BLOCKS] * 4
        + [pltpu.VMEM((nodes // Y_LO, 2 * b, LANES), short) for b in DY_BLOCKS],
        compiler_params=pltpu.CompilerParams(
            collective_id=1, has_side_effects=True, vmem_limit_bytes=48 * 1024 * 1024
        ),
        name="expert_gossip",
    )(*held)

    results = (mixed_gu.reshape(width, cols), mixed_down, mean_gu, mean_down)
    return pl.pallas_call(
        put_out,
        out_shape=tuple(jax.ShapeDtypeStruct(a.shape, a.dtype) for a in results),
        in_specs=[inside] * 4,
        out_specs=(outside,) * 4,
        scratch_shapes=[pltpu.SemaphoreType.DMA((13,))],
        compiler_params=pltpu.CompilerParams(vmem_limit_bytes=1024 * 1024),
        name="put_out",
    )(*results)


def solution(mesh):
    both = P(("node", "expert"), None)
    split = P("node", "expert")
    return jax.shard_map(
        step,
        mesh=mesh,
        in_specs=(split, split, both, both, both, P()),
        out_specs=(split, split, split, split),
        check_vma=False,
    )
```
